256 devices in a mesh: gx: 8 (over x, core), gy: 8 (over z), gz: 4 (over y).
Axes of the slice: x: 4, y: 4, z: 8, core: 2. Of those that a mesh axis runs over, the one named last changes fastest.
Arguments:
- local_displacement: float32 [8, 8, 4, 6, 128, 128], P('gx', 'gy', 'gz'), may hold values from -6 to 6
- coarse_load: float32 [8, 8, 4, 6, 128], P('gx', 'gy', 'gz'), may hold values from -12 to 12
- flexibility: float32 [8, 8, 4, 768, 768], P('gx', 'gy', 'gz'), as said below
- block_map: int32 [8, 8, 4, 768], P('gx', 'gy', 'gz'), may hold values from 0 to 767, each once within a row
- mode_counts: int32 [8, 8, 4], P('gx', 'gy', 'gz'), may hold values from 3 to 6, as said below
- mode_traces: float32 [8, 8, 4, 6, 6, 128], P('gx', 'gy', 'gz')
- coarse_rows: float32 [8, 8, 4, 6, 1536], P('gx', 'gy', 'gz'), as said below
- stored_dirs: float32 [8, 8, 4, 40, 6, 128], P('gx', 'gy', 'gz'), as said below
- stored_images: float32 [8, 8, 4, 40, 6, 128], P('gx', 'gy', 'gz'), as said below
- stored_curv: float32 [40], replicated, may hold values from 1 to 4
Outputs:
- multipliers: float32 [8, 8, 4, 6, 128, 128], P('gx', 'gy', 'gz')
- residual: float32 [8, 8, 4, 6, 128, 128], P('gx', 'gy', 'gz')
The draws below stay inside these ranges and needn't reach their ends.
Inputs may be any that keep to these rules, and one draw needn't show every extreme that they name: `flexibility`: each subdomain's matrix is symmetric positive definite. `coarse_rows`: read as a [1536, 1536] matrix it is exactly symmetric: the inverse of G^T G for the coarse basis G of the present modes, with ones added on the diagonal of absent modes. `mode_counts`: modes numbered from the count on are absent. `block_map`: each subdomain's row names every interface position once. `stored_dirs`: both copies of every face agree: slot 2a of a subdomain equals slot 2a+1 of its lower neighbour along grid dimension a. `stored_images`: both copies of every face agree: slot 2a of a subdomain equals slot 2a+1 of its lower neighbour along grid dimension a.
All inputs are finite; a program needn't handle non-finite values.
Results may differ from the reference program's by a relative error of at most 0.0003.
Values sent between devices are 32-bit elements; how exact they have to be, the bound alone decides.
A program may use at most 128 MiB of HBM per device.

```python
import math
import jax
import jax.numpy as jnp
from jax import lax

FACE = 128
RHS = 128
STORED = 40
RM = 6
ITERS = 3
NB = 768
SX = 8
SY = 8
SZ = 4
SUBS = 256
CMODES = 1536


def face_draw(draw_key, shape):
    return jax.random.normal(draw_key, shape, jnp.float32)


def coarse_bundle(key):
    counts = jax.random.randint(jax.random.fold_in(key, 101), (SX, SY, SZ), 3, RM + 1, dtype=jnp.int32)
    shared = face_draw(jax.random.fold_in(key, 102), (SX, SY, SZ, RM, 3, FACE))
    own_part = face_draw(jax.random.fold_in(key, 103), (SX, SY, SZ, RM, 6, FACE))
    slots = []
    for grid_dim in range(3):
        plus_face = shared[:, :, :, :, grid_dim]
        slots.append(jnp.roll(plus_face, 1, axis=grid_dim))
        slots.append(plus_face)
    traces = (jnp.stack(slots, axis=4) + 0.25 * own_part) * FACE ** (-0.5)
    present = (jnp.arange(RM, dtype=jnp.int32)[None, None, None, :] < counts[..., None]).astype(jnp.float32)
    masked = traces * present[..., None, None]
    diagonal_blocks = jnp.einsum('xyzmsf,xyznsf->xyzmn', masked, masked).reshape(SUBS, RM, RM)
    unit = jnp.eye(SUBS, dtype=jnp.float32)
    gram = jnp.einsum('st,smn->smtn', unit, diagonal_blocks)
    for grid_dim in range(3):
        above = jnp.roll(masked[:, :, :, :, 2 * grid_dim], -1, axis=grid_dim)
        coupling = -jnp.einsum('xyzmf,xyznf->xyzmn', masked[:, :, :, :, 2 * grid_dim + 1], above).reshape(SUBS, RM, RM)
        shifter = jnp.roll(unit.reshape(SX, SY, SZ, SUBS), -1, axis=grid_dim).reshape(SUBS, SUBS)
        gram = gram + jnp.einsum('st,smn->smtn', shifter, coupling) + jnp.einsum('st,smn->tnsm', shifter, coupling)
    absent = (1.0 - present).reshape(CMODES)
    matrix = gram.reshape(CMODES, CMODES) + jnp.diag(absent)
    inverse = jnp.linalg.inv(matrix)
    inverse = 0.5 * (inverse + inverse.T)
    return (counts, traces, inverse.reshape(SX, SY, SZ, RM, CMODES))


def draw_mode_counts(key, part):
    return coarse_bundle(key)[0]


def draw_mode_traces(key, part):
    return coarse_bundle(key)[1]


def draw_coarse_rows(key, part):
    return coarse_bundle(key)[2]


def stored_slabs(key, salt, spread):
    raw_key = jax.random.fold_in(key, salt)
    owned = jax.random.normal(raw_key, (SX, SY, SZ, STORED, 3, FACE), jnp.float32) * spread
    slots = []
    for grid_dim in range(3):
        plus_face = owned[:, :, :, :, grid_dim]
        slots.append(jnp.roll(plus_face, 1, axis=grid_dim))
        slots.append(plus_face)
    return jnp.stack(slots, axis=4)


def draw_stored_dirs(key, part):
    return stored_slabs(key, 201, 0.1)


def draw_stored_images(key, part):
    return stored_slabs(key, 202, (3.0 * FACE * SUBS) ** (-0.5))


def draw_flexibility(key, part):
    raw_key = jax.random.fold_in(key, 301)
    raw = jax.random.normal(raw_key, (SX, SY, SZ, NB, NB), jnp.float32)
    symmetric = (raw + jnp.swapaxes(raw, -1, -2)) * (0.35 / (2.0 * NB) ** 0.5)
    scales = jnp.exp(jax.random.uniform(jax.random.fold_in(key, 302), (SX, SY, SZ, NB), jnp.float32, jnp.log(0.7), jnp.log(1.4)))
    core = symmetric + jnp.eye(NB, dtype=jnp.float32)
    return core * (scales[..., :, None] * scales[..., None, :])


def block_levels(own_key, dims, pieces, low, high):
    gain, own = 1.0, jax.random.fold_in(own_key, 6)
    for dim, parts in pieces:
        draws = jnp.exp(jax.random.uniform(jax.random.fold_in(own, dim), (parts,), jnp.float32, low / len(pieces), high / len(pieces)))
        gain = gain * jnp.repeat(draws, dims[dim] // parts).reshape([-1 if axis == dim else 1 for axis in range(len(dims))])
    return gain


def normal_values(rng, extent, scale, most, shards=(), held_as=jnp.bfloat16):
    values = jax.random.normal(rng, extent, jnp.float32) * scale
    if len(shards) > 0:
        values = block_levels(rng, extent, shards, -0.22, 0.18) * values
    return jnp.clip(values, min=-most, max=most).astype(held_as)


def setup_inputs(seed: int = 0) -> dict:
    key_list = jax.random.split(jax.random.key(seed), 11)
    local_displacement = normal_values(key_list[0], (SX, SY, SZ, 6, FACE, RHS), 1.0, 6.0, ((0, 8), (1, 8), (2, 4)), jnp.float32)
    coarse_load = normal_values(key_list[1], (SX, SY, SZ, RM, RHS), 2.0, 12.0, ((0, 8), (1, 8), (2, 4)), jnp.float32)
    flexibility = draw_flexibility(jax.random.fold_in(key_list[10], 71), 0)
    block_map = jax.vmap(lambda own: jax.random.permutation(own, NB))(jax.random.split(key_list[3], SX * SY * SZ)).reshape((SX, SY, SZ, NB)).astype(jnp.int32)
    mode_counts = draw_mode_counts(jax.random.fold_in(key_list[10], 71), 0)
    mode_traces = draw_mode_traces(jax.random.fold_in(key_list[10], 71), 0)
    coarse_rows = draw_coarse_rows(jax.random.fold_in(key_list[10], 71), 0)
    stored_dirs = draw_stored_dirs(jax.random.fold_in(key_list[10], 71), 0)
    stored_images = draw_stored_images(jax.random.fold_in(key_list[10], 71), 0)
    stored_curv = jnp.clip(jnp.exp(jax.random.uniform(key_list[9], (STORED,), jnp.float32, math.log(1.0), math.log(4.0))), 1.0, 4.0)
    return {"local_displacement": local_displacement, "coarse_load": coarse_load, "flexibility": flexibility, "block_map": block_map, "mode_counts": mode_counts, "mode_traces": mode_traces, "coarse_rows": coarse_rows, "stored_dirs": stored_dirs, "stored_images": stored_images, "stored_curv": stored_curv}


precise = lax.Precision.HIGHEST

def assemble(field):
    slots = []
    for grid_dim in range(3):
        minus_side = field[:, :, :, 2 * grid_dim]
        plus_side = field[:, :, :, 2 * grid_dim + 1]
        slots.append(minus_side + jnp.roll(plus_side, 1, axis=grid_dim))
        slots.append(plus_side + jnp.roll(minus_side, -1, axis=grid_dim))
    return jnp.stack(slots, axis=3)

def single_apply(matrix, mapping, vector):
    picked = vector[mapping]
    product = jnp.dot(matrix, picked, precision=precise)
    return jnp.zeros_like(vector).at[mapping].set(product)

def flex_apply(flexibility, block_map, field):
    flat = field.reshape(SUBS, NB, RHS)
    result = jax.vmap(single_apply)(flexibility.reshape(SUBS, NB, NB), block_map.reshape(SUBS, NB), flat)
    return result.reshape(field.shape)

def coarse_solve(coarse_rows, loads):
    matrix = coarse_rows.reshape(CMODES, CMODES)
    return jnp.dot(matrix, loads.reshape(CMODES, RHS), precision=precise).reshape(SX, SY, SZ, RM, RHS)

def graph(signed, alpha):
    return assemble(jnp.einsum('xyzmsf,xyzmr->xyzsfr', signed, alpha, precision=precise))

def inner(first, second):
    return jnp.sum(first[:, :, :, 1::2] * second[:, :, :, 1::2], axis=(0, 1, 2, 3, 4))

def reference(local_displacement, coarse_load, flexibility, block_map, mode_counts, mode_traces, coarse_rows, stored_dirs, stored_images, stored_curv):
    signs = jnp.array([-1.0, 1.0, -1.0, 1.0, -1.0, 1.0], jnp.float32)
    field_signs = signs[:, None, None]
    present = (jnp.arange(RM, dtype=jnp.int32)[None, None, None, :] < mode_counts[..., None]).astype(jnp.float32)
    signed = mode_traces * present[..., None, None] * signs[:, None]

    def project(field):
        partial_loads = jnp.einsum('xyzmsf,xyzsfr->xyzmr', signed, field, precision=precise)
        return field - graph(signed, coarse_solve(coarse_rows, partial_loads))
    lam = graph(signed, coarse_solve(coarse_rows, coarse_load))
    moved = flex_apply(flexibility, block_map, field_signs * lam)
    resid = project(assemble(field_signs * (local_displacement - moved)))
    directions, images, curves = ([], [], [])
    for step in range(ITERS):
        stored_part = jnp.einsum('xyzisf,xyzsfr->ir', stored_images[:, :, :, :, 1::2], resid[:, :, :, 1::2], precision=precise)
        beta = stored_part / stored_curv[:, None]
        gammas = [inner(images[index], resid) / curves[index] for index in range(len(images))]
        direction = resid - jnp.einsum('xyzisf,ir->xyzsfr', stored_dirs, beta, precision=precise)
        for index in range(len(directions)):
            direction = direction - directions[index] * gammas[index]
        image_now = project(assemble(field_signs * flex_apply(flexibility, block_map, field_signs * direction)))
        curve = inner(direction, image_now)
        rate = inner(direction, resid) / curve
        lam = lam + rate * direction
        resid = resid - rate * image_now
        directions.append(direction)
        images.append(image_now)
        curves.append(curve)
    return (lam, resid)
```

```python
import functools

import jax
import jax.numpy as jnp
from jax import lax
from jax.experimental import pallas as pl
from jax.experimental.pallas import tpu as pltpu
from jax.sharding import PartitionSpec as P

F32, BF16 = jnp.float32, jnp.bfloat16
AXES = ("gx", "gy", "gz")
FACE = 128
NB = 6 * FACE
STORED = 40
STEPS = 5


def dot(a, b):
    return jnp.dot(a, b, preferred_element_type=F32)


def split(x):
    high = x.astype(BF16)
    return high, (x - high.astype(F32)).astype(BF16)


def wide(x):
    return jnp.concatenate(split(x), axis=1)


def fold(product, rows):
    half = product.shape[1] // 2
    return (product[:rows, :half] + product[:rows, half:]) + product[rows:, :half]


def thrice(x):
    high, low = split(x)
    high, low = high.astype(F32), low.astype(F32)
    return (high + pltpu.roll(low, STORED, 1) + pltpu.roll(high, 2 * STORED, 1)).astype(BF16)


def kernel(sizes, disp_hbm, load, flex_hbm, bmap, counts, traces, rows, dirs, images, curv, lam_out, res_out, s):
    nx, ny, nz = sizes
    me = dict(zip(AXES, (lax.axis_index(a) for a in AXES)))
    count = dict(zip(AXES, sizes))

    def other(axis, delta):
        return lax.rem(me[axis] + (count[axis] + delta), count[axis])

    barrier = pltpu.get_barrier_semaphore()
    for axis in AXES:
        for delta in range(1, count[axis]):
            pl.semaphore_signal(barrier, inc=1, device_id={axis: other(axis, delta)}, device_id_type=pl.DeviceIdType.MESH)

    fetch_flex = pltpu.make_async_copy(flex_hbm, s["flex"], s["local"].at[0])
    fetch_flex.start()
    fetch_disp = pltpu.make_async_copy(disp_hbm, s["disp"], s["local"].at[1])
    fetch_disp.start()

    used = [0]
    unsent = []

    def phase():
        used[0] += 1
        return s["sent"].at[used[0] - 1], s["came"].at[used[0] - 1]

    def wait_bytes(ref, sem):
        pltpu.make_async_copy(ref, ref, sem).wait()

    def send(src, dst, sems, target):
        pltpu.make_async_remote_copy(
            src_ref=src,
            dst_ref=dst,
            send_sem=sems[0],
            recv_sem=sems[1],
            device_id=target,
            device_id_type=pl.DeviceIdType.MESH,
        ).start()

    def finish(sems, ref):
        unsent.append((sems[0], ref))
        return lambda: wait_bytes(ref, sems[1])

    def to_faces(piece, dst):
        sems = phase()
        for slot in (2, 3, 4, 5, 0, 1):
            axis = AXES[slot // 2]
            target = {axis: other(axis, 1 if slot % 2 else -1)}
            send(piece(slot), dst.at[slot ^ 1], sems, target)
        return finish(sems, dst)

    def to_all(axis, src, dst):
        sems = phase()
        for delta in range(1, count[axis]):
            send(src, dst.at[me[axis]], sems, {axis: other(axis, delta)})
        return finish(sems, dst.at[pl.ds(0, count[axis] - 1)])

    def to_each(axis, src, dst):
        sems = phase()
        for delta in range(1, count[axis]):
            peer = other(axis, delta)
            send(src.at[peer], dst.at[me[axis]], sems, {axis: peer})
        return finish(sems, dst.at[pl.ds(0, count[axis] - 1)])

    def total(buf):
        out = buf[0]
        for j in range(1, buf.shape[0]):
            out = out + buf[j]
        return out

    own_rows, own_cut = s["own_rows"], s["cut"]
    own_rows[...] = jnp.zeros_like(own_rows)
    own_rows[0:6, :] = rows[...]
    group = nz * 6
    own_cut[...] = jnp.zeros_like(own_cut)
    for j in range(ny):
        for i in range(nx):
            at = (i * ny + j) * group
            own_cut[j, :, i * group : (i + 1) * group] = own_rows[:, at : at + group]

    present = lax.broadcasted_iota(jnp.int32, (6, FACE), 0) < counts[0, 0, 0]
    own_modes = s["own_modes"]
    own_modes[...] = jnp.zeros_like(own_modes)
    for slot in range(6):
        sign = 1.0 if slot % 2 else -1.0
        own_modes[slot, 0:6, :] = jnp.where(present, sign * traces[:, slot, :], 0.0)

    block = s["block0"]
    block[...] = jnp.zeros_like(block)
    block[0:6, :] = load[...]

    pl.semaphore_wait(barrier, nx + ny + nz - 3)

    def coarse_x(k, c):
        s[f"gx{k}"][me["gx"]] = c
        return to_all("gx", s[f"gx{k}"].at[me["gx"]], s[f"gx{k}"])

    def coarse_z(k):
        s[f"gz{k}"][me["gz"]] = s[f"gx{k}"][...]
        return to_all("gz", s[f"gx{k}"], s[f"gz{k}"])

    def coarse_y(k):
        width = s[f"gx{k}"].shape[-1]
        c = s[f"gz{k}"][...].reshape(nx * nz * 8, width)
        if width == FACE:
            partial = fold(dot(s["inverse"][...], wide(c)), ny * 8)
        else:
            partial = jnp.concatenate(
                [fold(dot(s["inverse"][...], wide(c[:, at : at + FACE])), ny * 8) for at in range(0, width, FACE)], axis=1
            )
        s[f"part{k}"][...] = partial.reshape(ny, 8, width)
        s[f"gy{k}"][me["gy"]] = s[f"part{k}"][me["gy"]]
        return to_each("gy", s[f"part{k}"], s[f"gy{k}"])

    def coarse_faces(k):
        s[f"alpha{k}"][...] = total(s[f"gy{k}"])
        return to_faces(lambda slot: s[f"alpha{k}"], s[f"near{k}"])

    def graph(k, slot, at=0):
        own = s[f"alpha{k}"][:, at : at + FACE]
        near = s[f"near{k}"][slot, :, at : at + FACE]
        a = jnp.concatenate([own, near], axis=0)
        high, low = split(a)
        high, low = high.astype(F32), low.astype(F32)
        stack = jnp.concatenate([high, high, low, jnp.zeros((FACE - 48, FACE), F32)], axis=0).astype(BF16)
        return dot(s["basis"][slot], stack)

    def face(ref, slot):
        return ref[slot * FACE : (slot + 1) * FACE, :]

    def modes_dot(z):
        return fold(dot(s["modes2"][...], wide(z)), 8)

    came_x = to_all("gx", block, s["gx0"])
    s["gx0"][me["gx"]] = block[...]
    came_cut = to_each("gy", own_cut, s["all_cut"])
    s["all_cut"][me["gy"]] = own_cut[me["gy"]]
    came_modes = to_faces(lambda slot: own_modes.at[slot], s["near_modes"])

    modes = jnp.concatenate([own_modes[slot] for slot in range(6)], axis=1)
    high, low = split(modes)
    s["modes2"][...] = jnp.concatenate([high.astype(F32), low.astype(F32)], axis=0).astype(BF16)

    fetch_flex.wait()

    def cut_flex(i, carry):
        at = pl.ds(pl.multiple_of(i * FACE, FACE), FACE)
        high, low = split(s["flex"][at, :])
        s["flex2"][at, 0:NB] = high
        s["flex2"][at, NB : 2 * NB] = low
        sign = lax.convert_element_type(2 * lax.rem(i, 2) - 1, F32)
        spot = i * FACE + lax.broadcasted_iota(jnp.int32, (FACE, NB), 0)
        s["pick"][at, :] = jnp.where(bmap[...] == spot, sign, 0.0).astype(BF16)
        return carry

    lax.fori_loop(0, 6, cut_flex, 0)

    def pick_rows(i, carry):
        at = pl.multiple_of(i * FACE, FACE)
        out = dot(s["pick"][pl.ds(at, FACE), :], s["flex2"][...])
        s["half"][pl.ds(at, FACE), :] = out[:, 0:NB].astype(BF16)
        s["half"][pl.ds(NB + at, FACE), :] = out[:, NB : 2 * NB].astype(BF16)
        return carry

    def pick_columns(i, carry):
        at = pl.ds(pl.multiple_of(i * FACE, FACE), FACE)
        out = lax.dot_general(
            s["half"][at, :], s["pick"][...], (((1,), (1,)), ((), ())), preferred_element_type=F32
        )
        s["op2"][at, :] = out.astype(BF16)
        return carry

    came_x()
    came_z = coarse_z(0)
    lax.fori_loop(0, 3, pick_rows, 0)

    came_cut()
    wide_cut = s["all_cut"][...].reshape(ny * 8, s["all_cut"].shape[-1])
    col = lax.broadcasted_iota(jnp.int32, (256, 256), 1)
    row = lax.broadcasted_iota(jnp.int32, (256, 256), 0)
    place = lax.rem(lax.div(col, 8), nx) * group + lax.div(col, 8 * nx) * 6 + lax.rem(col, 8)
    pick = jnp.where((row == place) & (lax.rem(col, 8) < 6), 1.0, 0.0).astype(BF16)
    high, low = split(wide_cut)
    s["inverse"][...] = dot(jnp.concatenate([high, low], axis=0), pick).astype(BF16)

    came_z()
    came_y = coarse_y(0)
    lax.fori_loop(3, 6, pick_rows, 0)
    lax.fori_loop(0, 6, pick_columns, 0)
    came_modes()
    for slot in range(6):
        both = jnp.concatenate([own_modes[slot], s["near_modes"][slot]], axis=0)
        high, low = split(both)
        high, low = high.astype(F32), low.astype(F32)
        tall = jnp.concatenate([high, low, high, jnp.zeros((FACE - 48, FACE), F32)], axis=0)
        s["basis"][slot] = tall.T.astype(BF16)
    came_y()
    came_faces = coarse_faces(0)
    lax.fori_loop(6, 12, pick_columns, 0)
    fetch_disp.wait()
    came_faces()
    lam = s["lam"]
    for slot in range(6):
        lam[slot * FACE : (slot + 1) * FACE, :] = graph(0, slot)

    def operate(k, x, given=None):
        out = fold(dot(s["op2"][...], wide(x)), NB)
        for slot in range(6):
            part = out[slot * FACE : (slot + 1) * FACE, :]
            if given is not None:
                part = (1.0 if slot % 2 else -1.0) * face(given, slot) - part
            s[f"out{k}"][slot] = part
        return to_faces(lambda slot: s[f"out{k}"].at[slot], s[f"in{k}"])

    def assembled(k):
        return (s[f"out{k}"][...] + s[f"in{k}"][...]).reshape(NB, FACE)

    came_halo = operate(1, lam[...], s["disp"])
    scale = s["scale"]
    scale[...] = jnp.ones_like(scale)
    scale[0:1, 0:STORED] = curv[...]
    inverse_curv = 1.0 / scale[0:1, :]
    field_d = s["field_d"]
    for slot in range(6):
        tall = jnp.concatenate([dirs[:, slot, :], jnp.zeros((FACE - STORED, FACE), F32)], axis=0)
        field_d[slot * FACE : (slot + 1) * FACE, :] = tall.T * inverse_curv
    s["dirs3"][...] = thrice(field_d[...])
    for j in range(3):
        high, low = split(images[:, 2 * j + 1, :])
        high, low = high.astype(F32), low.astype(F32)
        s["images2"][j] = jnp.concatenate([high, low], axis=0).astype(BF16)

    came_halo()
    z = s["z"]
    z[...] = assembled(1)
    came_x = coarse_x(1, modes_dot(z[...]))
    came_halo_d = operate(0, field_d[...])
    came_x()
    came_z = coarse_z(1)
    came_z()
    came_y = coarse_y(1)
    came_halo_d()
    zd = s["zd"]
    zd[...] = assembled(0)
    modes_d = modes_dot(zd[...])
    came_y()
    came_faces = coarse_faces(1)
    came_faces()
    w = s["w"]
    for slot in range(6):
        w[slot * FACE : (slot + 1) * FACE, :] = face(z, slot) - graph(1, slot)

    def odd_dot(a, b):
        out = None
        for slot in (1, 3, 5):
            part = jnp.sum(face(a, slot) * face(b, slot), axis=0, keepdims=True)
            out = part if out is None else out + part
        return out

    def stored_dot(a):
        out = None
        for j, slot in enumerate((1, 3, 5)):
            part = dot(s["images2"][j], wide(face(a, slot)))
            out = part if out is None else out + part
        return fold(out, STORED)

    def superstep(k, v, pairs, extra=None):
        came_halo = operate(k, v[...])
        sums = s[f"sums{k}"]
        lines = [odd_dot(a, b) for a, b in pairs]
        lines.append(jnp.zeros((8 - len(lines), FACE), F32))
        flat = jnp.concatenate([stored_dot(v), jnp.concatenate(lines, axis=0), jnp.zeros((16, FACE), F32)], axis=0)
        sums[...] = flat.reshape(8, 8, FACE)
        s[f"sx{k}"][me["gx"]] = sums[me["gx"]]
        came_sx = to_each("gx", sums, s[f"sx{k}"])
        came_halo()
        z[...] = assembled(k)
        c = modes_dot(z[...])
        if extra is not None:
            c = jnp.concatenate([c, extra], axis=1)
        came_x = coarse_x(k, c)
        came_sx()
        s[f"sz{k}"][me["gz"]] = total(s[f"sx{k}"])
        came_sz = to_all("gz", s[f"sz{k}"].at[me["gz"]], s[f"sz{k}"])
        came_x()
        came_z = coarse_z(k)
        came_sz()
        s[f"sy{k}"][me["gy"]] = total(s[f"sz{k}"])
        came_sy = to_all("gy", s[f"sy{k}"].at[me["gy"]], s[f"sy{k}"])
        came_z()
        came_y = coarse_y(k)
        came_sy()
        s[f"all{k}"][me["gx"]] = total(s[f"sy{k}"])
        came_all = to_all("gx", s[f"all{k}"].at[me["gx"]], s[f"all{k}"])
        came_y()
        came_faces = coarse_faces(k)
        came_all()
        return came_faces, s[f"all{k}"][...].reshape(64, FACE)

    def stored_part(gram):
        high, low = split(gram)
        high, low = high.astype(F32), low.astype(F32)
        return jnp.concatenate([high, high, low, jnp.zeros((8, FACE), F32)], axis=0).astype(BF16)

    came_faces, sums = superstep(2, w, (), extra=modes_d)
    gram = sums[0:STORED]
    stack = stored_part(gram)
    p, q, paw = (s["p0"], s["p1"], s["p2"]), (s["q0"], s["q1"], s["q2"]), s["paw"]
    p[0][...] = w[...] - dot(s["dirs3"][...], stack)
    came_faces()
    for slot in range(6):
        at = slice(slot * FACE, (slot + 1) * FACE)
        paw[at, :] = face(z, slot) - graph(2, slot)
        s["pad3"][at, :] = thrice(face(zd, slot) - graph(2, slot, FACE))
    q[0][...] = paw[...] - dot(s["pad3"][...], stack)

    own, curves = [], []
    for k in range(2):
        pairs = [(p[k], q[k]), (p[k], w), (q[k], w), (q[k], q[k])]
        pairs += [(q[j], q[k]) for j in range(k)]
        came_faces, sums = superstep(3 + k, q[k], pairs)
        lines = [sums[STORED + j : STORED + j + 1] for j in range(len(pairs))]
        curves.append(lines[0])
        rate = lines[1] / lines[0]
        own = [own[j] - rate * lines[4 + j] for j in range(k)] + [lines[2] - rate * lines[3]]
        gammas = [own[j] / curves[j] for j in range(k + 1)]
        gram = gram - rate * sums[0:STORED]
        stack = stored_part(gram)
        lam[...] = lam[...] + rate * p[k][...]
        w[...] = w[...] - rate * q[k][...]
        new = w[...] - dot(s["dirs3"][...], stack)
        off = dot(s["pad3"][...], stack)
        for j in range(k + 1):
            new = new - p[j][...] * gammas[j]
            off = off + q[j][...] * gammas[j]
        p[k + 1][...] = new
        q[k + 1][...] = off
        came_faces()
        for slot in range(6):
            at = slice(slot * FACE, (slot + 1) * FACE)
            fresh = paw[at, :] - rate * (face(z, slot) - graph(3 + k, slot))
            paw[at, :] = fresh
            q[k + 1][at, :] = fresh - q[k + 1][at, :]

    lines = jnp.concatenate([odd_dot(p[2], q[2]), odd_dot(p[2], w), jnp.zeros((6, FACE), F32)], axis=0)
    for axis in ("gx", "gz", "gy"):
        buf = s["end_" + axis]
        buf[me[axis]] = lines
        to_all(axis, buf.at[me[axis]], buf)()
        lines = total(buf)
    rate = lines[1:2] / lines[0:1]
    lam_out[...] = lam[...] + rate * p[2][...]
    res_out[...] = w[...] - rate * q[2][...]

    for sem, ref in unsent:
        wait_bytes(ref, sem)


def per_device(sizes, disp, load, flex, bmap, counts, traces, rows, dirs, images, curv):
    nx, ny, nz = sizes
    vmem = pltpu.VMEM
    shapes = {
        "flex": vmem((NB, NB), F32),
        "disp": vmem((NB, FACE), F32),
        "flex2": vmem((NB, 2 * NB), BF16),
        "pick": vmem((NB, NB), BF16),
        "half": vmem((2 * NB, NB), BF16),
        "op2": vmem((2 * NB, NB), BF16),
        "own_rows": vmem((8, 6 * nx * ny * nz), F32),
        "cut": vmem((ny, 8, 256), F32),
        "all_cut": vmem((ny, 8, 256), F32),
        "inverse": vmem((2 * ny * 8, nx * nz * 8), BF16),
        "own_modes": vmem((6, 8, FACE), F32),
        "near_modes": vmem((6, 8, FACE), F32),
        "modes2": vmem((16, NB), BF16),
        "basis": vmem((6, FACE, FACE), BF16),
        "block0": vmem((8, FACE), F32),
        "scale": vmem((8, FACE), F32),
        "dirs3": vmem((NB, FACE), BF16),
        "pad3": vmem((NB, FACE), BF16),
        "images2": vmem((3, 2 * STORED, FACE), BF16),
        "end_gx": vmem((nx, 8, FACE), F32),
        "end_gy": vmem((ny, 8, FACE), F32),
        "end_gz": vmem((nz, 8, FACE), F32),
        "local": pltpu.SemaphoreType.DMA((2,)),
        "sent": pltpu.SemaphoreType.DMA((64,)),
        "came": pltpu.SemaphoreType.DMA((64,)),
    }
    for name in ("lam", "w", "z", "zd", "field_d", "paw", "p0", "p1", "p2", "q0", "q1", "q2"):
        shapes[name] = vmem((NB, FACE), F32)
    for k in range(STEPS):
        width = 2 * FACE if k == 2 else FACE
        shapes[f"out{k}"] = vmem((6, FACE, FACE), F32)
        shapes[f"in{k}"] = vmem((6, FACE, FACE), F32)
        shapes[f"gx{k}"] = vmem((nx, 8, width), F32)
        shapes[f"gz{k}"] = vmem((nz, nx, 8, width), F32)
        shapes[f"part{k}"] = vmem((ny, 8, width), F32)
        shapes[f"gy{k}"] = vmem((ny, 8, width), F32)
        shapes[f"alpha{k}"] = vmem((8, width), F32)
        shapes[f"near{k}"] = vmem((6, 8, width), F32)
        if k >= 2:
            shapes[f"sums{k}"] = vmem((nx, 8, FACE), F32)
            shapes[f"sx{k}"] = vmem((nx, 8, FACE), F32)
            shapes[f"sz{k}"] = vmem((nz, 8, FACE), F32)
            shapes[f"sy{k}"] = vmem((ny, 8, FACE), F32)
            shapes[f"all{k}"] = vmem((nx, 8, FACE), F32)
    names = list(shapes)

    def body(*refs):
        kernel(sizes, *refs[:12], dict(zip(names, refs[12:])))

    inside = pl.BlockSpec(memory_space=pltpu.VMEM)
    outside = pl.BlockSpec(memory_space=pltpu.HBM)
    lam, res = pl.pallas_call(
        body,
        out_shape=[jax.ShapeDtypeStruct((NB, FACE), F32)] * 2,
        in_specs=[
            outside,
            inside,
            outside,
            inside,
            pl.BlockSpec(memory_space=pltpu.SMEM),
            inside,
            inside,
            inside,
            inside,
            inside,
        ],
        out_specs=[inside, inside],
        scratch_shapes=[shapes[n] for n in names],
        compiler_params=pltpu.CompilerParams(
            collective_id=0, has_side_effects=True, vmem_limit_bytes=56 * 1024 * 1024
        ),
        name="feti",
    )(
        disp.reshape(NB, FACE),
        load.reshape(6, FACE),
        flex.reshape(NB, NB),
        bmap.reshape(1, NB),
        counts,
        traces.reshape(6, 6, FACE),
        rows.reshape(6, -1),
        dirs.reshape(STORED, 6, FACE),
        images.reshape(STORED, 6, FACE),
        curv.reshape(1, STORED),
    )
    shape = (1, 1, 1, 6, FACE, FACE)
    return lam.reshape(shape), res.reshape(shape)


def solution(mesh):
    sizes = tuple(mesh.shape[a] for a in AXES)
    cut = P("gx", "gy", "gz")
    return jax.shard_map(
        functools.partial(per_device, sizes),
        mesh=mesh,
        in_specs=(cut,) * 9 + (P(),),
        out_specs=(cut, cut),
        check_vma=False,
    )
```

```python
import functools
from types import SimpleNamespace

import jax
import jax.numpy as jnp
from jax import lax
from jax.experimental import pallas as pl
from jax.experimental.pallas import tpu as pltpu
from jax.sharding import PartitionSpec as P

F32, BF16 = jnp.float32, jnp.bfloat16
GX, GY, GZ = AXES = ("gx", "gy", "gz")
FACE = 128
NB = 6 * FACE
STORED = 40
STEPS = 5
ACROSS = tuple(tuple((1 if slot % 2 else -1) if axis == slot // 2 else 0 for axis in range(3)) for slot in range(6))
ZERO = (0, 0, 0)


def plus(a, b):
    return tuple(i + j for i, j in zip(a, b))


RING = tuple(dict.fromkeys((ZERO, *ACROSS, *(plus(a, b) for a in ACROSS for b in ACROSS))))


def dot(a, b):
    return jnp.dot(a, b, preferred_element_type=F32)


def split(x):
    high = x.astype(BF16)
    return high, (x - high.astype(F32)).astype(BF16)


def wide(x):
    return jnp.concatenate(split(x), axis=1)


def fold(product, rows):
    half = product.shape[1] // 2
    return (product[:rows, :half] + product[:rows, half:]) + product[rows:, :half]


def thrice(x):
    high, low = split(x)
    high, low = high.astype(F32), low.astype(F32)
    return (high + pltpu.roll(low, STORED, 1) + pltpu.roll(high, 2 * STORED, 1)).astype(BF16)


def kernel(sizes, given, lam_out, dir_out, res_out, image_out, rate_out, s):
    nx, ny, nz = sizes
    me = dict(zip(AXES, (lax.axis_index(a) for a in AXES)))
    count = dict(zip(AXES, sizes))
    mesh_id = pl.DeviceIdType.MESH

    def other(axis, delta):
        return lax.rem(me[axis] + (count[axis] + delta), count[axis])

    def at_offset(offset):
        return {axis: other(axis, d) for axis, d in zip(AXES, offset) if d}

    plane = [(dx, 0, dz) for dx in range(nx) for dz in range(nz) if dx or dz]
    line = [(0, dy, 0) for dy in range(1, ny)]
    corner = [o for o in RING if o[1] and (o[0] or o[2])]

    barrier = pltpu.get_barrier_semaphore()
    peers = [at_offset(o) for o in line + plane + corner]
    for peer in peers:
        pl.semaphore_signal(barrier, inc=1, device_id=peer, device_id_type=mesh_id)

    got = s.given
    fetch = {
        name: pltpu.make_async_copy(given[name], got[name], s.local.at[j]) for j, name in enumerate(given)
    }
    for copy in fetch.values():
        copy.start()
    fetch, got = SimpleNamespace(**fetch), SimpleNamespace(**got)

    used = [0]
    unsent = []

    def phase():
        used[0] += 1
        return s.sent.at[used[0] - 1], s.came.at[used[0] - 1]

    def wait_bytes(ref, sem):
        pltpu.make_async_copy(ref, ref, sem).wait()

    def send(src, dst, sems, target):
        pltpu.make_async_remote_copy(
            src_ref=src, dst_ref=dst, send_sem=sems[0], recv_sem=sems[1], device_id=target, device_id_type=mesh_id
        ).start()

    def finish(sems, ref):
        unsent.append((sems[0], ref))
        return lambda: wait_bytes(ref, sems[1])

    def to_faces(piece, dst):
        sems = phase()
        for slot in (2, 3, 4, 5, 0, 1):
            send(piece(slot), dst.at[slot ^ 1], sems, at_offset(ACROSS[slot]))
        return finish(sems, dst)

    def to_all(axis, value, dst):
        sems = phase()
        dst[me[axis]] = value
        for delta in range(1, count[axis]):
            send(dst.at[me[axis]], dst.at[me[axis]], sems, {axis: other(axis, delta)})
        return finish(sems, dst.at[pl.ds(0, count[axis] - 1)])

    def to_each(axis, src, dst):
        sems = phase()
        for delta in range(1, count[axis]):
            peer = other(axis, delta)
            send(src.at[peer], dst.at[me[axis]], sems, {axis: peer})
        dst[me[axis]] = src[me[axis]]
        return finish(sems, dst.at[pl.ds(0, count[axis] - 1)])

    def to_plane(value, dst):
        spot = me[GZ] * nx + me[GX]
        dst[spot] = value
        sems = phase()
        for o in plane:
            send(dst.at[spot], dst.at[spot], sems, at_offset(o))
        return finish(sems, dst.at[pl.ds(0, len(plane))])

    def to_ring(value, dst, reach=len(RING)):
        dst[0] = value
        sems = phase()
        for j in range(1, reach):
            send(dst.at[0], dst.at[j], sems, at_offset(tuple(-d for d in RING[j])))
        return finish(sems, dst.at[pl.ds(1, reach - 1)])

    def total(buf):
        out = buf[0]
        for j in range(1, buf.shape[0]):
            out = out + buf[j]
        return out

    def halves(x):
        high, low = split(x)
        return high.astype(F32), low.astype(F32)

    def slot_rows(slot):
        return slice(slot * FACE, (slot + 1) * FACE)

    def face(ref, slot):
        return ref[slot_rows(slot), :]

    group = nz * 6
    s.own_rows[...] = jnp.zeros_like(s.own_rows)
    s.cut[...] = jnp.zeros_like(s.cut)
    fetch.rows.wait()
    s.own_rows[0:6, :] = got.rows[:, 0, :]
    for j in range(ny):
        for i in range(nx):
            at = (i * ny + j) * group
            s.cut[j, :, i * group : (i + 1) * group] = s.own_rows[:, at : at + group]

    fetch.counts.wait()
    fetch.traces.wait()
    present = lax.broadcasted_iota(jnp.int32, (6, FACE), 0) < got.counts[...]
    own_modes = s.own_modes
    own_modes[...] = jnp.zeros_like(own_modes)
    for slot in range(6):
        sign = 1.0 if slot % 2 else -1.0
        own_modes[slot, 0:6, :] = jnp.where(present, sign * got.traces[:, slot, 0, :], 0.0)

    fetch.load.wait()
    s.block0[...] = jnp.zeros_like(s.block0)
    s.block0[0:6, :] = got.load[:, 0, :]

    pl.semaphore_wait(barrier, len(peers))

    def by_lanes(width, f):
        parts = [f(slice(at, at + FACE)) for at in range(0, width, FACE)]
        return parts[0] if len(parts) == 1 else jnp.concatenate(parts, axis=1)

    def coarse_y(k):
        width = s.plane[k].shape[-1]
        c = s.plane[k][...].reshape(nx * nz * 8, width)
        partial = by_lanes(width, lambda at: fold(dot(s.inverse[...], wide(c[:, at])), ny * 8))
        s.part[k][...] = partial.reshape(ny, 8, width)
        return to_each(GY, s.part[k], s.gy[k])

    def graph(k, slot, at=slice(0, FACE)):
        own = s.ring[k][0, :, at]
        near = s.ring[k][1 + slot, :, at]
        high, low = halves(jnp.concatenate([own, near], axis=0))
        stack = jnp.concatenate([high, high, low, jnp.zeros((FACE - 48, FACE), F32)], axis=0).astype(BF16)
        return dot(s.basis[slot], stack)

    def modes_dot(z):
        return fold(dot(s.modes2[...], wide(z)), 8)

    def apply(x):
        return fold(dot(s.op2[...], wide(x)), NB)

    def spread(r, k):
        own = None
        for slot in range(6):
            part = fold(dot(s.both2[slot], wide(r[slot_rows(slot), :])), 16)
            own = part[0:8] if own is None else own + part[0:8]
            s.share[k][slot] = part[8:16]
        came = to_faces(lambda slot: s.share[k].at[slot], s.shares[k])
        s.mine[k][...] = own
        return came

    def gathered(k):
        return s.mine[k][...] + total(s.shares[k])

    def stencil(k):
        width = s.ring[k].shape[-1]
        a = s.ring[k][...].reshape(256, width)
        return by_lanes(width, lambda at: fold(dot(s.stencil2[...], wide(a[:, at])), 8))

    def operate(k, x, load=None):
        out = apply(x)
        for slot in range(6):
            part = out[slot_rows(slot), :]
            if load is not None:
                part = (1.0 if slot % 2 else -1.0) * face(load, slot) - part
            s.out[k][slot] = part
        return to_faces(lambda slot: s.out[k].at[slot], s.halo[k])

    def assembled(k):
        return (s.out[k][...] + s.halo[k][...]).reshape(NB, FACE)

    came_cut = to_each(GY, s.cut, s.all_cut)
    came_plane = to_plane(s.block0[...], s.plane[0])
    came_modes = to_faces(lambda slot: own_modes.at[slot], s.near_modes)

    modes = jnp.concatenate([own_modes[slot] for slot in range(6)], axis=1)
    s.modes2[...] = jnp.concatenate(halves(modes), axis=0).astype(BF16)
    for k in range(STEPS - 1):
        tail = s.ring[k].shape
        s.ring[k][len(RING) :] = jnp.zeros((tail[0] - len(RING), *tail[1:]), F32)

    fetch.flex.wait()
    fetch.bmap.wait()

    def cut_flex(i, carry):
        at = pl.ds(pl.multiple_of(i * FACE, FACE), FACE)
        high, low = split(got.flex[at, :])
        s.flex2[at, 0:NB] = high
        s.flex2[at, NB : 2 * NB] = low
        sign = lax.convert_element_type(2 * lax.rem(i, 2) - 1, F32)
        spot = i * FACE + lax.broadcasted_iota(jnp.int32, (FACE, NB), 0)
        s.pick[at, :] = jnp.where(got.bmap[...] == spot, sign, 0.0).astype(BF16)
        return carry

    def pick_rows(i, carry):
        at = pl.multiple_of(i * FACE, FACE)
        out = dot(s.pick[pl.ds(at, FACE), :], s.flex2[...])
        s.half[pl.ds(at, FACE), :] = out[:, 0:NB].astype(BF16)
        s.half[pl.ds(NB + at, FACE), :] = out[:, NB : 2 * NB].astype(BF16)
        return carry

    def pick_columns(i, carry):
        at = pl.ds(pl.multiple_of(i * 2 * FACE, 2 * FACE), 2 * FACE)
        out = lax.dot_general(s.half[at, :], s.pick[...], (((1,), (1,)), ((), ())), preferred_element_type=F32)
        s.op2[at, :] = out.astype(BF16)
        return carry

    lax.fori_loop(0, 6, cut_flex, 0)
    lax.fori_loop(0, 6, pick_rows, 0)

    came_cut()
    wide_cut = s.all_cut[...].reshape(ny * 8, s.all_cut.shape[-1])
    col = lax.broadcasted_iota(jnp.int32, (256, 256), 1)
    row = lax.broadcasted_iota(jnp.int32, (256, 256), 0)
    place = lax.rem(lax.div(col, 8), nx) * group + lax.div(col, 8 * nx) * 6 + lax.rem(col, 8)
    pick = jnp.where((row == place) & (lax.rem(col, 8) < 6), 1.0, 0.0).astype(BF16)
    s.inverse[...] = dot(jnp.concatenate(split(wide_cut), axis=0), pick).astype(BF16)

    lax.fori_loop(0, 6, pick_columns, 0)
    came_plane()
    came_y = coarse_y(0)

    came_modes()
    for slot in range(6):
        own, near = own_modes[slot], s.near_modes[slot]
        high, low = halves(jnp.concatenate([own, near], axis=0))
        s.both2[slot] = jnp.concatenate([high, low], axis=0).astype(BF16)
        tall = jnp.concatenate([high, low, high, jnp.zeros((FACE - 48, FACE), F32)], axis=0)
        s.basis[slot] = tall.T.astype(BF16)
        blank = [own] + [jnp.zeros((8, FACE), F32)] * 15
        blank[1 + slot] = near
        s.field_g[slot_rows(slot), :] = jnp.concatenate(blank, axis=0).T
    came_share = spread(apply(s.field_g[...]), 0)
    fetch.disp.wait()
    signed = [(1.0 if slot % 2 else -1.0) * face(got.disp, slot) for slot in range(6)]
    came_load = spread(jnp.concatenate(signed, axis=0), 1)
    came_y()
    came_ring = to_ring(total(s.gy[0]), s.ring[0])

    came_share()
    lane = lax.broadcasted_iota(jnp.int32, (8, FACE), 1)
    parts = [jnp.zeros((8, FACE), F32)] * 2
    for j, base in enumerate((ZERO, *ACROSS)):
        source = s.mine[0][...] if j == 0 else s.shares[0][j - 1]
        for b, step in enumerate((ZERO, *ACROSS)):
            to = RING.index(plus(base, step))
            moved = pltpu.roll(source, (8 * (to % 16) - 8 * b) % FACE, 1)
            parts[to // 16] = parts[to // 16] + jnp.where(lax.div(lane, 8) == to % 16, moved, 0.0)
    s.stencil2[...] = jnp.concatenate(halves(jnp.concatenate(parts, axis=1)), axis=0).astype(BF16)
    came_load()
    came_ring()
    came_plane = to_plane(gathered(1) - stencil(0), s.plane[1])

    lam, w, z, zd, paw = s.lam, s.w, s.z, s.zd, s.paw
    for slot in range(6):
        lam[slot_rows(slot), :] = graph(0, slot)
    came_halo = operate(1, lam[...], got.disp)
    fetch.dirs.wait()
    fetch.curv.wait()
    fetch.images.wait()
    s.scale[...] = jnp.ones_like(s.scale)
    s.scale[0:1, 0:STORED] = got.curv[...]
    inverse_curv = 1.0 / s.scale[0:1, :]
    for slot in range(6):
        tall = jnp.concatenate([got.dirs[slot], jnp.zeros((FACE - STORED, FACE), F32)], axis=0)
        s.field_d[slot_rows(slot), :] = tall.T * inverse_curv
    came_halo_d = operate(0, s.field_d[...])
    came_plane()
    came_y = coarse_y(1)
    came_halo()
    z[...] = assembled(1)
    came_share = spread(apply(z[...]), 2)
    s.dirs3[...] = thrice(s.field_d[...])
    for j in range(3):
        s.images2[j] = jnp.concatenate(halves(got.images[2 * j + 1]), axis=0).astype(BF16)
    came_y()
    came_ring = to_ring(total(s.gy[1]), s.ring[1])
    came_halo_d()
    zd[...] = assembled(0)
    modes_d = modes_dot(zd[...])
    came_share()
    start = gathered(2)
    came_ring()
    came_plane = to_plane(jnp.concatenate([start - stencil(1), modes_d], axis=1), s.plane[2])
    for slot in range(6):
        w[slot_rows(slot), :] = face(z, slot) - graph(1, slot)

    def odd_dot(a, b):
        out = None
        for slot in (1, 3, 5):
            part = jnp.sum(face(a, slot) * face(b, slot), axis=0, keepdims=True)
            out = part if out is None else out + part
        return out

    def stored_dot(a):
        out = None
        for j, slot in enumerate((1, 3, 5)):
            part = dot(s.images2[j], wide(face(a, slot)))
            out = part if out is None else out + part
        return fold(out, STORED)

    def superstep(k, v, pairs, came_plane):
        j = k - 2
        lines = [odd_dot(a, b) for a, b in pairs]
        lines.append(jnp.zeros((8 - len(lines), FACE), F32))
        flat = jnp.concatenate([stored_dot(v), *lines, jnp.zeros((16, FACE), F32)], axis=0)
        s.sums[j][...] = flat.reshape(8, 8, FACE)
        came_sums = to_each(GY, s.sums[j], s.sums_y[j])
        came_halo = operate(k, v[...])
        came_plane()
        came_y = coarse_y(k)
        came_sums()
        came_sums = to_plane(total(s.sums_y[j]), s.sums_plane[j])
        came_d = spread(apply(zd[...]), 3) if k == 2 else None
        came_halo()
        z[...] = assembled(k)
        came_share = spread(apply(z[...]), k + 2) if k < 4 else None
        came_y()
        came_ring = to_ring(total(s.gy[k]), s.ring[k], len(RING) if k < 4 else 7)
        came_sums()
        came_sums = to_all(GY, total(s.sums_plane[j]), s.sums_all[j])
        for came in (came_d, came_share):
            if came is not None:
                came()
        return came_ring, came_sums, s.sums_all[j]

    def stored_part(gram):
        high, low = halves(gram)
        return jnp.concatenate([high, high, low, jnp.zeros((8, FACE), F32)], axis=0).astype(BF16)

    p, q = s.p, s.q
    came_ring, came_sums, sums = superstep(2, w, (), came_plane)
    came_ring()
    off = stencil(2)
    modes_paw = gathered(4) - off[:, 0:FACE]
    modes_pad3 = thrice(gathered(3) - off[:, FACE:])
    for slot in range(6):
        at = slot_rows(slot)
        paw[at, :] = face(z, slot) - graph(2, slot)
        s.pad3[at, :] = thrice(face(zd, slot) - graph(2, slot, slice(FACE, 2 * FACE)))
    came_sums()
    gram = sums[...].reshape(64, FACE)[0:STORED]
    stack = stored_part(gram)
    modes_q = [modes_paw - dot(modes_pad3, stack)]
    came_plane = to_plane(modes_q[0], s.plane[3])
    q[0][...] = paw[...] - dot(s.pad3[...], stack)
    p[0][...] = w[...] - dot(s.dirs3[...], stack)

    own, curves = [], []
    for k in range(2):
        pairs = [(p[k], q[k]), (p[k], w), (q[k], w), (q[k], q[k])]
        pairs += [(q[j], q[k]) for j in range(k)]
        came_ring, came_sums, sums = superstep(3 + k, q[k], pairs, came_plane)
        if k == 0:
            came_ring()
            change = gathered(5) - stencil(3)
        came_sums()
        sums = sums[...].reshape(64, FACE)
        lines = [sums[STORED + j : STORED + j + 1] for j in range(len(pairs))]
        curves.append(lines[0])
        rate = lines[1] / lines[0]
        own = [own[j] - rate * lines[4 + j] for j in range(k)] + [lines[2] - rate * lines[3]]
        gammas = [own[j] / curves[j] for j in range(k + 1)]
        gram = gram - rate * sums[0:STORED]
        stack = stored_part(gram)
        if k == 0:
            modes_paw = modes_paw - rate * change
            came_plane = to_plane(modes_paw - dot(modes_pad3, stack) - gammas[0] * modes_q[0], s.plane[4])
            for slot in range(6):
                at = slot_rows(slot)
                paw[at, :] = paw[at, :] - rate * (face(z, slot) - graph(3, slot))
        lam[...] = lam[...] + rate * p[k][...]
        w[...] = w[...] - rate * q[k][...]
        new = w[...] - dot(s.dirs3[...], stack)
        off = dot(s.pad3[...], stack)
        for j in range(k + 1):
            new = new - p[j][...] * gammas[j]
            off = off + q[j][...] * gammas[j]
        p[k + 1][...] = new
        if k == 0:
            q[1][...] = paw[...] - off

    over = rate * jnp.sum(modes_dot(p[2][...]) * s.ring[4][0], axis=0, keepdims=True)
    q[2][...] = paw[...] - off
    for slot in (1, 3, 5):
        known = face(q[2], slot) - rate * face(z, slot)
        over = over + jnp.sum(face(p[2], slot) * known, axis=0, keepdims=True)
    lines = jnp.concatenate([over, odd_dot(p[2], w), jnp.zeros((6, FACE), F32)], axis=0)
    came_end = to_plane(lines, s.end_plane)
    came_ring()
    for slot in range(6):
        at = slot_rows(slot)
        image_out[at, :] = q[2][at, :] - rate * (face(z, slot) - graph(4, slot))

    lam_out[...] = lam[...]
    dir_out[...] = p[2][...]
    res_out[...] = w[...]
    came_end()
    to_all(GY, total(s.end_plane), s.end_gy)()
    lines = total(s.end_gy)
    rate_out[...] = lines[1:2] / lines[0:1]

    for sem, ref in unsent:
        wait_bytes(ref, sem)


def per_device(sizes, disp, load, flex, bmap, counts, traces, rows, dirs, images, curv):
    nx, ny, nz = sizes
    vmem = pltpu.VMEM
    given = dict(
        rows=rows.reshape(6, 1, -1),
        load=load.reshape(6, 1, FACE),
        counts=counts.reshape(1, 1),
        traces=traces.reshape(6, 6, 1, FACE),
        flex=flex.reshape(NB, NB),
        bmap=bmap.reshape(1, NB),
        disp=disp.reshape(NB, FACE),
        dirs=dirs.reshape(STORED, 6, FACE).swapaxes(0, 1),
        curv=curv.reshape(1, STORED),
        images=images.reshape(STORED, 6, FACE).swapaxes(0, 1),
    )
    widths = [2 * FACE if k == 2 else FACE for k in range(STEPS)]
    field = vmem((NB, FACE), F32)
    blocks = lambda n, width=FACE: vmem((n, 8, width), F32)
    scratch = dict(
        given={name: vmem(x.shape, x.dtype) for name, x in given.items()},
        flex2=vmem((NB, 2 * NB), BF16),
        pick=vmem((NB, NB), BF16),
        half=vmem((2 * NB, NB), BF16),
        op2=vmem((2 * NB, NB), BF16),
        own_rows=vmem((8, 6 * nx * ny * nz), F32),
        cut=blocks(ny, 256),
        all_cut=blocks(ny, 256),
        inverse=vmem((2 * ny * 8, nx * nz * 8), BF16),
        own_modes=blocks(6),
        near_modes=blocks(6),
        modes2=vmem((16, NB), BF16),
        both2=vmem((6, 32, FACE), BF16),
        stencil2=vmem((16, 256), BF16),
        basis=vmem((6, FACE, FACE), BF16),
        block0=vmem((8, FACE), F32),
        scale=vmem((8, FACE), F32),
        dirs3=vmem((NB, FACE), BF16),
        pad3=vmem((NB, FACE), BF16),
        images2=vmem((3, 2 * STORED, FACE), BF16),
        end_plane=blocks(nx * nz),
        end_gy=blocks(ny),
        lam=field,
        w=field,
        z=field,
        zd=field,
        field_d=field,
        field_g=field,
        paw=field,
        p=[field] * 3,
        q=[field] * 3,
        out=[vmem((6, FACE, FACE), F32)] * STEPS,
        halo=[vmem((6, FACE, FACE), F32)] * STEPS,
        plane=[blocks(nx * nz, width) for width in widths],
        part=[blocks(ny, width) for width in widths],
        gy=[blocks(ny, width) for width in widths],
        ring=[blocks(32, width) for width in widths],
        share=[blocks(6)] * 6,
        shares=[blocks(6)] * 6,
        mine=[vmem((8, FACE), F32)] * 6,
        sums=[blocks(ny)] * 3,
        sums_y=[blocks(ny)] * 3,
        sums_plane=[blocks(nx * nz)] * 3,
        sums_all=[blocks(ny)] * 3,
        local=pltpu.SemaphoreType.DMA((len(given),)),
        sent=pltpu.SemaphoreType.DMA((64,)),
        came=pltpu.SemaphoreType.DMA((64,)),
    )
    leaves, tree = jax.tree.flatten(scratch, is_leaf=lambda x: not isinstance(x, (dict, list)))

    def body(*refs):
        cut = len(given)
        held = SimpleNamespace(**jax.tree.unflatten(tree, refs[cut + 5 :]))
        kernel(sizes, dict(zip(given, refs[:cut])), *refs[cut : cut + 5], held)

    inside = pl.BlockSpec(memory_space=pltpu.VMEM)
    outside = pl.BlockSpec(memory_space=pltpu.HBM)
    lam, direction, res, image, rate = pl.pallas_call(
        body,
        out_shape=[jax.ShapeDtypeStruct((NB, FACE), F32)] * 4 + [jax.ShapeDtypeStruct((1, FACE), F32)],
        in_specs=[outside] * len(given),
        out_specs=[inside] * 5,
        scratch_shapes=leaves,
        compiler_params=pltpu.CompilerParams(
            collective_id=0, has_side_effects=True, vmem_limit_bytes=56 * 1024 * 1024
        ),
        name="feti",
    )(*given.values())
    shape = (1, 1, 1, 6, FACE, FACE)
    return (lam + rate * direction).reshape(shape), (res - rate * image).reshape(shape)


def solution(mesh):
    sizes = tuple(mesh.shape[a] for a in AXES)
    cut = P("gx", "gy", "gz")
    return jax.shard_map(
        functools.partial(per_device, sizes),
        mesh=mesh,
        in_specs=(cut,) * 9 + (P(),),
        out_specs=(cut, cut),
        check_vma=False,
    )
```

```python
import functools
from types import SimpleNamespace

import jax
import jax.numpy as jnp
from jax import lax
from jax.experimental import pallas as pl
from jax.experimental.pallas import tpu as pltpu
from jax.sharding import PartitionSpec as P

F32, BF16 = jnp.float32, jnp.bfloat16
GX, GY, GZ = AXES = ("gx", "gy", "gz")
FACE = 128
NB = 6 * FACE
STORED = 40
STEPS = 6
STORED_STEP = 5
ACROSS = tuple(tuple((1 if slot % 2 else -1) if axis == slot // 2 else 0 for axis in range(3)) for slot in range(6))
ZERO = (0, 0, 0)


def plus(a, b):
    return tuple(i + j for i, j in zip(a, b))


RING = tuple(dict.fromkeys((ZERO, *ACROSS, *(plus(a, b) for a in ACROSS for b in ACROSS))))


def dot(a, b):
    return jnp.dot(a, b, preferred_element_type=F32)


def split(x):
    high = x.astype(BF16)
    return high, (x - high.astype(F32)).astype(BF16)


def wide(x):
    return jnp.concatenate(split(x), axis=1)


def fold(product, rows):
    half = product.shape[1] // 2
    return (product[:rows, :half] + product[:rows, half:]) + product[rows:, :half]


def thrice(x):
    high, low = split(x)
    high, low = high.astype(F32), low.astype(F32)
    return (high + pltpu.roll(low, STORED, 1) + pltpu.roll(high, 2 * STORED, 1)).astype(BF16)


def kernel(sizes, given, lam_out, dir_out, res_out, image_out, rate_out, s):
    nx, ny, nz = sizes
    me = dict(zip(AXES, (lax.axis_index(a) for a in AXES)))
    count = dict(zip(AXES, sizes))
    mesh_id = pl.DeviceIdType.MESH

    def other(axis, delta):
        return lax.rem(me[axis] + (count[axis] + delta), count[axis])

    def at_offset(offset):
        return {axis: other(axis, d) for axis, d in zip(AXES, offset) if d}

    plane = [(dx, 0, dz) for dx in range(nx) for dz in range(nz) if dx or dz]
    line = [(0, dy, 0) for dy in range(1, ny)]
    corner = [o for o in RING if o[1] and (o[0] or o[2])]

    barrier = pltpu.get_barrier_semaphore()
    peers = [at_offset(o) for o in line + plane + corner]
    for peer in peers:
        pl.semaphore_signal(barrier, inc=1, device_id=peer, device_id_type=mesh_id)

    got = s.given
    fetch = {
        name: pltpu.make_async_copy(given[name], got[name], s.local.at[j]) for j, name in enumerate(given)
    }
    for copy in fetch.values():
        copy.start()
    fetch, got = SimpleNamespace(**fetch), SimpleNamespace(**got)

    used = [0]
    unsent = []

    def phase():
        used[0] += 1
        return s.sent.at[used[0] - 1], s.came.at[used[0] - 1]

    def wait_bytes(ref, sem):
        pltpu.make_async_copy(ref, ref, sem).wait()

    def send(src, dst, sems, target):
        pltpu.make_async_remote_copy(
            src_ref=src, dst_ref=dst, send_sem=sems[0], recv_sem=sems[1], device_id=target, device_id_type=mesh_id
        ).start()

    def finish(sems, ref):
        unsent.append((sems[0], ref))
        return lambda: wait_bytes(ref, sems[1])

    def to_faces(piece, dst):
        sems = phase()
        for slot in (2, 3, 4, 5, 0, 1):
            send(piece(slot), dst.at[slot ^ 1], sems, at_offset(ACROSS[slot]))
        return finish(sems, dst)

    def to_all(axis, value, dst):
        sems = phase()
        dst[me[axis]] = value
        for delta in range(1, count[axis]):
            send(dst.at[me[axis]], dst.at[me[axis]], sems, {axis: other(axis, delta)})
        return finish(sems, dst.at[pl.ds(0, count[axis] - 1)])

    def to_each(axis, src, dst):
        sems = phase()
        for delta in range(1, count[axis]):
            peer = other(axis, delta)
            send(src.at[peer], dst.at[me[axis]], sems, {axis: peer})
        dst[me[axis]] = src[me[axis]]
        return finish(sems, dst.at[pl.ds(0, count[axis] - 1)])

    def to_plane(value, dst):
        spot = me[GZ] * nx + me[GX]
        dst[spot] = value
        sems = phase()
        for o in plane:
            send(dst.at[spot], dst.at[spot], sems, at_offset(o))
        return finish(sems, dst.at[pl.ds(0, len(plane))])

    def to_ring(value, dst, reach=len(RING)):
        dst[0] = value
        sems = phase()
        for j in range(1, reach):
            send(dst.at[0], dst.at[j], sems, at_offset(tuple(-d for d in RING[j])))
        return finish(sems, dst.at[pl.ds(1, reach - 1)])

    def total(buf):
        out = buf[0]
        for j in range(1, buf.shape[0]):
            out = out + buf[j]
        return out

    def halves(x):
        high, low = split(x)
        return high.astype(F32), low.astype(F32)

    def slot_rows(slot):
        return slice(slot * FACE, (slot + 1) * FACE)

    def face(ref, slot):
        return ref[slot_rows(slot), :]

    group = nz * 6
    s.own_rows[...] = jnp.zeros_like(s.own_rows)
    s.cut[...] = jnp.zeros_like(s.cut)
    fetch.rows.wait()
    s.own_rows[0:6, :] = got.rows[:, 0, :]
    for j in range(ny):
        for i in range(nx):
            at = (i * ny + j) * group
            s.cut[j, :, i * group : (i + 1) * group] = s.own_rows[:, at : at + group]

    fetch.counts.wait()
    fetch.traces.wait()
    present = lax.broadcasted_iota(jnp.int32, (6, FACE), 0) < got.counts[...]
    own_modes = s.own_modes
    own_modes[...] = jnp.zeros_like(own_modes)
    for slot in range(6):
        sign = 1.0 if slot % 2 else -1.0
        own_modes[slot, 0:6, :] = jnp.where(present, sign * got.traces[:, slot, 0, :], 0.0)

    fetch.load.wait()
    s.block0[...] = jnp.zeros_like(s.block0)
    s.block0[0:6, :] = got.load[:, 0, :]

    pl.semaphore_wait(barrier, len(peers))

    def coarse_y(k):
        c = s.plane[k][...].reshape(nx * nz * 8, FACE)
        s.part[k][...] = fold(dot(s.inverse[...], wide(c)), ny * 8).reshape(ny, 8, FACE)
        return to_each(GY, s.part[k], s.gy[k])

    def graph(k, slot):
        own = s.ring[k][0]
        near = s.ring[k][1 + slot]
        high, low = halves(jnp.concatenate([own, near], axis=0))
        stack = jnp.concatenate([high, high, low, jnp.zeros((FACE - 48, FACE), F32)], axis=0).astype(BF16)
        return dot(s.basis[slot], stack)

    def modes_dot(z):
        return fold(dot(s.modes2[...], wide(z)), 8)

    def apply(x):
        return fold(dot(s.op2[...], wide(x)), NB)

    def spread(r, k):
        own = None
        for slot in range(6):
            part = fold(dot(s.both2[slot], wide(r[slot_rows(slot), :])), 16)
            own = part[0:8] if own is None else own + part[0:8]
            s.share[k][slot] = part[8:16]
        came = to_faces(lambda slot: s.share[k].at[slot], s.shares[k])
        s.mine[k][...] = own
        return came

    def gathered(k):
        return s.mine[k][...] + total(s.shares[k])

    def stencil(k):
        return fold(dot(s.stencil2[...], wide(s.ring[k][...].reshape(256, FACE))), 8)

    def operate(k, x, load=None):
        out = apply(x)
        for slot in range(6):
            part = out[slot_rows(slot), :]
            if load is not None:
                part = (1.0 if slot % 2 else -1.0) * face(load, slot) - part
            s.out[k][slot] = part
        return to_faces(lambda slot: s.out[k].at[slot], s.halo[k])

    def assembled(k):
        return (s.out[k][...] + s.halo[k][...]).reshape(NB, FACE)

    came_cut = to_each(GY, s.cut, s.all_cut)
    came_plane = to_plane(s.block0[...], s.plane[0])
    came_modes = to_faces(lambda slot: own_modes.at[slot], s.near_modes)

    modes = jnp.concatenate([own_modes[slot] for slot in range(6)], axis=1)
    s.modes2[...] = jnp.concatenate(halves(modes), axis=0).astype(BF16)
    for k in (0, 1, 2, 3, STORED_STEP):
        tail = s.ring[k].shape
        s.ring[k][len(RING) :] = jnp.zeros((tail[0] - len(RING), *tail[1:]), F32)

    fetch.flex.wait()
    fetch.bmap.wait()

    def cut_flex(i, carry):
        at = pl.ds(pl.multiple_of(i * FACE, FACE), FACE)
        high, low = split(got.flex[at, :])
        s.flex2[at, 0:NB] = high
        s.flex2[at, NB : 2 * NB] = low
        sign = lax.convert_element_type(2 * lax.rem(i, 2) - 1, F32)
        spot = i * FACE + lax.broadcasted_iota(jnp.int32, (FACE, NB), 0)
        s.pick[at, :] = jnp.where(got.bmap[...] == spot, sign, 0.0).astype(BF16)
        return carry

    def pick_rows(i, carry):
        at = pl.multiple_of(i * FACE, FACE)
        out = dot(s.pick[pl.ds(at, FACE), :], s.flex2[...])
        s.half[pl.ds(at, FACE), :] = out[:, 0:NB].astype(BF16)
        s.half[pl.ds(NB + at, FACE), :] = out[:, NB : 2 * NB].astype(BF16)
        return carry

    def pick_columns(i, carry):
        at = pl.ds(pl.multiple_of(i * 2 * FACE, 2 * FACE), 2 * FACE)
        out = lax.dot_general(s.half[at, :], s.pick[...], (((1,), (1,)), ((), ())), preferred_element_type=F32)
        s.op2[at, :] = out.astype(BF16)
        return carry

    lax.fori_loop(0, 6, cut_flex, 0)
    lax.fori_loop(0, 6, pick_rows, 0)
    lax.fori_loop(0, 6, pick_columns, 0)

    came_cut()
    wide_cut = s.all_cut[...].reshape(ny * 8, s.all_cut.shape[-1])
    col = lax.broadcasted_iota(jnp.int32, (256, 256), 1)
    row = lax.broadcasted_iota(jnp.int32, (256, 256), 0)
    place = lax.rem(lax.div(col, 8), nx) * group + lax.div(col, 8 * nx) * 6 + lax.rem(col, 8)
    pick = jnp.where((row == place) & (lax.rem(col, 8) < 6), 1.0, 0.0).astype(BF16)
    s.inverse[...] = dot(jnp.concatenate(split(wide_cut), axis=0), pick).astype(BF16)

    came_plane()
    came_y = coarse_y(0)

    came_modes()
    for slot in range(6):
        own, near = own_modes[slot], s.near_modes[slot]
        high, low = halves(jnp.concatenate([own, near], axis=0))
        s.both2[slot] = jnp.concatenate([high, low], axis=0).astype(BF16)
        tall = jnp.concatenate([high, low, high, jnp.zeros((FACE - 48, FACE), F32)], axis=0)
        s.basis[slot] = tall.T.astype(BF16)
        blank = [own] + [jnp.zeros((8, FACE), F32)] * 15
        blank[1 + slot] = near
        s.field_g[slot_rows(slot), :] = jnp.concatenate(blank, axis=0).T
    came_share = spread(apply(s.field_g[...]), 0)
    fetch.disp.wait()
    signed = [(1.0 if slot % 2 else -1.0) * face(got.disp, slot) for slot in range(6)]
    came_load = spread(jnp.concatenate(signed, axis=0), 1)
    came_y()
    came_ring = to_ring(total(s.gy[0]), s.ring[0])

    came_share()
    lane = lax.broadcasted_iota(jnp.int32, (8, FACE), 1)
    parts = [jnp.zeros((8, FACE), F32)] * 2
    for j, base in enumerate((ZERO, *ACROSS)):
        source = s.mine[0][...] if j == 0 else s.shares[0][j - 1]
        for b, step in enumerate((ZERO, *ACROSS)):
            to = RING.index(plus(base, step))
            moved = pltpu.roll(source, (8 * (to % 16) - 8 * b) % FACE, 1)
            parts[to // 16] = parts[to // 16] + jnp.where(lax.div(lane, 8) == to % 16, moved, 0.0)
    s.stencil2[...] = jnp.concatenate(halves(jnp.concatenate(parts, axis=1)), axis=0).astype(BF16)
    came_load()
    came_ring()
    came_plane = to_plane(gathered(1) - stencil(0), s.plane[1])

    lam, w, z, zd, paw = s.lam, s.w, s.z, s.zd, s.paw
    for slot in range(6):
        lam[slot_rows(slot), :] = graph(0, slot)
    came_halo = operate(1, lam[...], got.disp)
    fetch.dirs.wait()
    fetch.curv.wait()
    fetch.images.wait()
    s.scale[...] = jnp.ones_like(s.scale)
    s.scale[0:1, 0:STORED] = got.curv[...]
    inverse_curv = 1.0 / s.scale[0:1, :]
    for slot in range(6):
        tall = jnp.concatenate([got.dirs[slot], jnp.zeros((FACE - STORED, FACE), F32)], axis=0)
        s.field_d[slot_rows(slot), :] = tall.T * inverse_curv
    came_halo_d = operate(0, s.field_d[...])
    came_plane()
    came_y = coarse_y(1)
    came_halo()
    z[...] = assembled(1)
    came_share = spread(apply(z[...]), 2)
    came_halo_d()
    zd[...] = assembled(0)
    came_plane_d = to_plane(modes_dot(zd[...]), s.plane[STORED_STEP])
    s.dirs3[...] = thrice(s.field_d[...])
    modes_of_images = None
    for slot in range(6):
        tall = jnp.concatenate([own_modes[slot], jnp.zeros((FACE - 8, FACE), F32)], axis=0)
        part = lax.dot_general(
            got.images[slot],
            tall,
            (((1,), (1,)), ((), ())),
            precision=lax.Precision.HIGHEST,
            preferred_element_type=F32,
        )
        modes_of_images = part if slot == 0 else modes_of_images + part
        if slot % 2:
            s.images2[slot // 2] = jnp.concatenate(halves(got.images[slot]), axis=0).astype(BF16)
    s.images2[3] = jnp.concatenate(halves(modes_of_images), axis=0).astype(BF16)

    class StoredSums:
        def __init__(self, j, field, alpha):
            self.j = j
            parts = [field[slot_rows(slot), :] for slot in (1, 3, 5)]
            parts.append(jnp.concatenate([-alpha, jnp.zeros((FACE - 8, FACE), F32)], axis=0))
            out = None
            for i, part in enumerate(parts):
                term = dot(s.images2[i], wide(part))
                out = term if out is None else out + term
            flat = jnp.concatenate([fold(out, STORED), jnp.zeros((64 - STORED, FACE), F32)], axis=0)
            s.sums[j][...] = flat.reshape(8, 8, FACE)
            self.came = to_each(GY, s.sums[j], s.sums_y[j])

        def share(self):
            self.came()
            self.came = to_plane(total(s.sums_y[self.j]), s.sums_plane[self.j])

        def collect(self):
            self.came()
            self.came = to_all(GY, total(s.sums_plane[self.j]), s.sums_all[self.j])

        def result(self):
            self.came()
            return s.sums_all[self.j][...].reshape(64, FACE)[0:STORED]

    came_y()
    alpha = total(s.gy[1])
    came_ring = to_ring(alpha, s.ring[1])
    sums_w = StoredSums(0, z[...], alpha)
    came_share()
    start = gathered(2)
    came_ring()
    came_plane = to_plane(start - stencil(1), s.plane[2])
    for slot in range(6):
        w[slot_rows(slot), :] = face(z, slot) - graph(1, slot)

    def odd_dot(a, b):
        out = None
        for slot in (1, 3, 5):
            part = jnp.sum(face(a, slot) * face(b, slot), axis=0, keepdims=True)
            out = part if out is None else out + part
        return out

    def superstep(k, v, pairs, came_plane, sums):
        j = k - 3
        came_pairs, came_d, came_share, sums_d, sums_z = None, None, None, None, None
        if pairs:
            lines = [odd_dot(a, b) for a, b in pairs]
            lines.append(jnp.zeros((8 - len(lines), FACE), F32))
            came_pairs = to_all(GY, jnp.concatenate(lines, axis=0), s.pairs_y[j])
        sums[0].share()
        came_halo = operate(k, v[...])
        if k == 2:
            came_plane_d()
            came_y_d = coarse_y(STORED_STEP)
        came_plane()
        came_y = coarse_y(k)
        if pairs:
            came_pairs()
            came_pairs = to_plane(total(s.pairs_y[j]), s.pairs_plane[j])
        for each in sums:
            each.collect()
        if k == 2:
            came_d = spread(apply(zd[...]), 3)
        came_halo()
        z[...] = assembled(k)
        if k == 2:
            came_y_d()
            alpha = total(s.gy[STORED_STEP])
            came_ring_d = to_ring(alpha, s.ring[STORED_STEP])
            sums_d = StoredSums(1, zd[...], alpha)
        if k < 4:
            came_share = spread(apply(z[...]), k + 2)
        came_y()
        alpha = total(s.gy[k])
        came_ring = to_ring(alpha, s.ring[k], len(RING) if k < 4 else 7)
        if k < 4:
            sums_z = StoredSums(k, z[...], alpha)
        if k == 2:
            sums_d.share()
            came_d()
            came_ring_d()
        if k < 4:
            came_share()
        return came_ring, came_pairs, [x for x in (sums_z, sums_d) if x is not None]

    def stored_part(gram):
        high, low = halves(gram)
        return jnp.concatenate([high, high, low, jnp.zeros((8, FACE), F32)], axis=0).astype(BF16)

    p, q = s.p, s.q
    came_ring, _, later = superstep(2, w, (), came_plane, [sums_w])
    modes_pad3 = thrice(gathered(3) - stencil(STORED_STEP))
    gram = sums_w.result()
    stack = stored_part(gram)
    modes_off = gathered(4) - dot(modes_pad3, stack)
    came_ring()
    change = stencil(2)
    modes_q = modes_off - change
    modes_paw = gathered(4) - change
    came_plane = to_plane(modes_q, s.plane[3])
    for slot in range(6):
        at = slot_rows(slot)
        paw[at, :] = face(z, slot) - graph(2, slot)
        s.pad3[at, :] = thrice(face(zd, slot) - graph(STORED_STEP, slot))
    q[0][...] = paw[...] - dot(s.pad3[...], stack)
    p[0][...] = w[...] - dot(s.dirs3[...], stack)

    own, curves = [], []
    for k in range(2):
        pairs = [(p[k], q[k]), (p[k], w), (q[k], w), (q[k], q[k])]
        pairs += [(q[j], q[k]) for j in range(k)]
        came_ring, came_pairs, latest = superstep(3 + k, q[k], pairs, came_plane, later)
        came_pairs()
        sums = total(s.pairs_plane[k])
        lines = [sums[j : j + 1] for j in range(len(pairs))]
        if k == 0:
            gram_paw = later[0].result()
            gram_pad3 = thrice(later[1].result())
            gram_q = gram_paw - dot(gram_pad3, stack)
        else:
            gram_paw = gram_paw - rate * later[0].result()
            gram_q = gram_paw - dot(gram_pad3, stack) - gammas[0] * gram_q
        later = latest
        curves.append(lines[0])
        rate = lines[1] / lines[0]
        own = [own[j] - rate * lines[4 + j] for j in range(k)] + [lines[2] - rate * lines[3]]
        gammas = [own[j] / curves[j] for j in range(k + 1)]
        gram = gram - rate * gram_q
        stack = stored_part(gram)
        if k == 0:
            modes_off = modes_paw - rate * gathered(5) - dot(modes_pad3, stack) - gammas[0] * modes_q
        w[...] = w[...] - rate * q[k][...]
        new = w[...] - dot(s.dirs3[...], stack)
        off = dot(s.pad3[...], stack)
        for j in range(k + 1):
            new = new - p[j][...] * gammas[j]
            off = off + q[j][...] * gammas[j]
        p[k + 1][...] = new
        lam[...] = lam[...] + rate * p[k][...]
        if k == 0:
            q[1][...] = paw[...] - rate * z[...] - off
            came_ring()
            came_plane = to_plane(modes_off + rate * stencil(3), s.plane[4])
            for slot in range(6):
                at = slot_rows(slot)
                change = rate * graph(3, slot)
                paw[at, :] = paw[at, :] - rate * face(z, slot) + change
                q[1][at, :] = q[1][at, :] + change

    over = rate * jnp.sum(modes_dot(p[2][...]) * s.ring[4][0], axis=0, keepdims=True)
    q[2][...] = paw[...] - off
    for slot in (1, 3, 5):
        known = face(q[2], slot) - rate * face(z, slot)
        over = over + jnp.sum(face(p[2], slot) * known, axis=0, keepdims=True)
    lines = jnp.concatenate([over, odd_dot(p[2], w), jnp.zeros((6, FACE), F32)], axis=0)
    came_end = to_plane(lines, s.end_plane)
    came_ring()
    for slot in range(6):
        at = slot_rows(slot)
        image_out[at, :] = q[2][at, :] - rate * (face(z, slot) - graph(4, slot))

    lam_out[...] = lam[...]
    dir_out[...] = p[2][...]
    res_out[...] = w[...]
    came_end()
    to_all(GY, total(s.end_plane), s.end_gy)()
    lines = total(s.end_gy)
    rate_out[...] = lines[1:2] / lines[0:1]

    for sem, ref in unsent:
        wait_bytes(ref, sem)


def per_device(sizes, disp, load, flex, bmap, counts, traces, rows, dirs, images, curv):
    nx, ny, nz = sizes
    vmem = pltpu.VMEM
    given = dict(
        rows=rows.reshape(6, 1, -1),
        load=load.reshape(6, 1, FACE),
        counts=counts.reshape(1, 1),
        traces=traces.reshape(6, 6, 1, FACE),
        flex=flex.reshape(NB, NB),
        bmap=bmap.reshape(1, NB),
        disp=disp.reshape(NB, FACE),
        dirs=dirs.reshape(STORED, 6, FACE).swapaxes(0, 1),
        curv=curv.reshape(1, STORED),
        images=images.reshape(STORED, 6, FACE).swapaxes(0, 1),
    )
    field = vmem((NB, FACE), F32)
    blocks = lambda n, width=FACE: vmem((n, 8, width), F32)
    scratch = dict(
        given={name: vmem(x.shape, x.dtype) for name, x in given.items()},
        flex2=vmem((NB, 2 * NB), BF16),
        pick=vmem((NB, NB), BF16),
        half=vmem((2 * NB, NB), BF16),
        op2=vmem((2 * NB, NB), BF16),
        own_rows=vmem((8, 6 * nx * ny * nz), F32),
        cut=blocks(ny, 256),
        all_cut=blocks(ny, 256),
        inverse=vmem((2 * ny * 8, nx * nz * 8), BF16),
        own_modes=blocks(6),
        near_modes=blocks(6),
        modes2=vmem((16, NB), BF16),
        both2=vmem((6, 32, FACE), BF16),
        stencil2=vmem((16, 256), BF16),
        basis=vmem((6, FACE, FACE), BF16),
        block0=vmem((8, FACE), F32),
        scale=vmem((8, FACE), F32),
        dirs3=vmem((NB, FACE), BF16),
        pad3=vmem((NB, FACE), BF16),
        images2=vmem((4, 2 * STORED, FACE), BF16),
        end_plane=blocks(nx * nz),
        end_gy=blocks(ny),
        lam=field,
        w=field,
        z=field,
        zd=field,
        field_d=field,
        field_g=field,
        paw=field,
        p=[field] * 3,
        q=[field] * 3,
        out=[vmem((6, FACE, FACE), F32)] * STEPS,
        halo=[vmem((6, FACE, FACE), F32)] * STEPS,
        plane=[blocks(nx * nz)] * STEPS,
        part=[blocks(ny)] * STEPS,
        gy=[blocks(ny)] * STEPS,
        ring=[blocks(32)] * STEPS,
        share=[blocks(6)] * 6,
        shares=[blocks(6)] * 6,
        mine=[vmem((8, FACE), F32)] * 6,
        sums=[blocks(ny)] * 4,
        sums_y=[blocks(ny)] * 4,
        sums_plane=[blocks(nx * nz)] * 4,
        sums_all=[blocks(ny)] * 4,
        pairs_y=[blocks(ny)] * 2,
        pairs_plane=[blocks(nx * nz)] * 2,
        local=pltpu.SemaphoreType.DMA((len(given),)),
        sent=pltpu.SemaphoreType.DMA((64,)),
        came=pltpu.SemaphoreType.DMA((64,)),
    )
    leaves, tree = jax.tree.flatten(scratch, is_leaf=lambda x: not isinstance(x, (dict, list)))

    def body(*refs):
        cut = len(given)
        held = SimpleNamespace(**jax.tree.unflatten(tree, refs[cut + 5 :]))
        kernel(sizes, dict(zip(given, refs[:cut])), *refs[cut : cut + 5], held)

    inside = pl.BlockSpec(memory_space=pltpu.VMEM)
    outside = pl.BlockSpec(memory_space=pltpu.HBM)
    lam, direction, res, image, rate = pl.pallas_call(
        body,
        out_shape=[jax.ShapeDtypeStruct((NB, FACE), F32)] * 4 + [jax.ShapeDtypeStruct((1, FACE), F32)],
        in_specs=[outside] * len(given),
        out_specs=[inside] * 5,
        scratch_shapes=leaves,
        compiler_params=pltpu.CompilerParams(
            collective_id=0, has_side_effects=True, vmem_limit_bytes=56 * 1024 * 1024
        ),
        name="feti",
    )(*given.values())
    shape = (1, 1, 1, 6, FACE, FACE)
    return (lam + rate * direction).reshape(shape), (res - rate * image).reshape(shape)


def solution(mesh):
    sizes = tuple(mesh.shape[a] for a in AXES)
    cut = P("gx", "gy", "gz")
    return jax.shard_map(
        functools.partial(per_device, sizes),
        mesh=mesh,
        in_specs=(cut,) * 9 + (P(),),
        out_specs=(cut, cut),
        check_vma=False,
    )
```

```python
import functools
from types import SimpleNamespace

import jax
import jax.numpy as jnp
from jax import lax
from jax.experimental import pallas as pl
from jax.experimental.pallas import tpu as pltpu
from jax.sharding import PartitionSpec as P

F32, BF16 = jnp.float32, jnp.bfloat16
GX, GY, GZ = AXES = ("gx", "gy", "gz")
FACE = 128
NB = 6 * FACE
STORED = 40
STEPS = 6
STORED_STEP = 5
ACROSS = tuple(tuple((1 if slot % 2 else -1) if axis == slot // 2 else 0 for axis in range(3)) for slot in range(6))
ZERO = (0, 0, 0)


def plus(a, b):
    return tuple(i + j for i, j in zip(a, b))


RING = tuple(dict.fromkeys((ZERO, *ACROSS, *(plus(a, b) for a in ACROSS for b in ACROSS))))


def dot(a, b):
    return jnp.dot(a, b, preferred_element_type=F32)


def split(x):
    high = x.astype(BF16)
    return high, (x - high.astype(F32)).astype(BF16)


def wide(x):
    return jnp.concatenate(split(x), axis=1)


def fold(product, rows):
    half = product.shape[1] // 2
    return (product[:rows, :half] + product[:rows, half:]) + product[rows:, :half]


def thrice(x):
    high, low = split(x)
    high, low = high.astype(F32), low.astype(F32)
    return (high + pltpu.roll(low, STORED, 1) + pltpu.roll(high, 2 * STORED, 1)).astype(BF16)


def kernel(sizes, given, lam_out, dir_out, res_out, image_out, rate_out, s):
    nx, ny, nz = sizes
    me = dict(zip(AXES, (lax.axis_index(a) for a in AXES)))
    count = dict(zip(AXES, sizes))
    mesh_id = pl.DeviceIdType.MESH

    def other(axis, delta):
        return lax.rem(me[axis] + (count[axis] + delta), count[axis])

    def at_offset(offset):
        return {axis: other(axis, d) for axis, d in zip(AXES, offset) if d}

    def nearness(offset):
        x, y, z = (min(d % n, -d % n) for d, n in zip(offset, sizes))
        return -(x / 2 + y + z)

    plane = sorted(((dx, 0, dz) for dx in range(nx) for dz in range(nz) if dx or dz), key=nearness)
    line = sorted(((0, dy, 0) for dy in range(1, ny)), key=nearness)
    corner = [o for o in RING if o[1] and (o[0] or o[2])]

    barrier = pltpu.get_barrier_semaphore()
    peers = [at_offset(o) for o in line + plane + corner]
    for peer in peers:
        pl.semaphore_signal(barrier, inc=1, device_id=peer, device_id_type=mesh_id)

    got = s.given
    fetch = {
        name: pltpu.make_async_copy(given[name], got[name], s.local.at[j]) for j, name in enumerate(given)
    }
    for copy in fetch.values():
        copy.start()
    fetch, got = SimpleNamespace(**fetch), SimpleNamespace(**got)

    used = [0]
    unsent = []

    def phase():
        used[0] += 1
        return s.sent.at[used[0] - 1], s.came.at[used[0] - 1]

    def wait_bytes(ref, sem):
        pltpu.make_async_copy(ref, ref, sem).wait()

    def send(src, dst, sems, target):
        pltpu.make_async_remote_copy(
            src_ref=src, dst_ref=dst, send_sem=sems[0], recv_sem=sems[1], device_id=target, device_id_type=mesh_id
        ).start()

    def finish(sems, ref):
        unsent.append((sems[0], ref))
        return lambda: wait_bytes(ref, sems[1])

    def to_faces(piece, dst):
        sems = phase()
        for slot in (2, 3, 4, 5, 0, 1):
            send(piece(slot), dst.at[slot ^ 1], sems, at_offset(ACROSS[slot]))
        return finish(sems, dst)

    def to_all(value, dst):
        sems = phase()
        dst[me[GY]] = value
        for _, delta, _ in line:
            send(dst.at[me[GY]], dst.at[me[GY]], sems, {GY: other(GY, delta)})
        return finish(sems, dst.at[pl.ds(0, ny - 1)])

    def to_each(src, dst):
        sems = phase()
        for _, delta, _ in line:
            peer = other(GY, delta)
            send(src.at[peer], dst.at[me[GY]], sems, {GY: peer})
        dst[me[GY]] = src[me[GY]]
        return finish(sems, dst.at[pl.ds(0, ny - 1)])

    def to_plane(value, dst):
        spot = me[GZ] * nx + me[GX]
        dst[spot] = value
        sems = phase()
        for o in plane:
            send(dst.at[spot], dst.at[spot], sems, at_offset(o))
        return finish(sems, dst.at[pl.ds(0, len(plane))])

    def to_ring(value, dst, reach=len(RING)):
        dst[0] = value
        sems = phase()
        for j in sorted(range(1, reach), key=lambda j: nearness(RING[j])):
            send(dst.at[0], dst.at[j], sems, at_offset(tuple(-d for d in RING[j])))
        return finish(sems, dst.at[pl.ds(1, reach - 1)])

    def total(buf):
        out = buf[0]
        for j in range(1, buf.shape[0]):
            out = out + buf[j]
        return out

    def halves(x):
        high, low = split(x)
        return high.astype(F32), low.astype(F32)

    def eight(x):
        shape = list(x.shape)
        shape[-2] = 8 - shape[-2]
        return jnp.concatenate([x, jnp.zeros(shape, F32)], axis=x.ndim - 2)

    def slot_rows(slot):
        return slice(slot * FACE, (slot + 1) * FACE)

    def face(ref, slot):
        return ref[slot_rows(slot), :]

    group = nz * 6
    s.cut[...] = jnp.zeros_like(s.cut)
    fetch.rows.wait()
    s.own_rows[...] = got.rows[:, 0, :]
    for j in range(ny):
        for i in range(nx):
            at = (i * ny + j) * group
            s.cut[j, :, i * group : (i + 1) * group] = s.own_rows[:, at : at + group]

    fetch.counts.wait()
    fetch.traces.wait()
    present = lax.broadcasted_iota(jnp.int32, (6, FACE), 0) < got.counts[...]
    own_modes = s.own_modes
    own_modes[...] = jnp.zeros_like(own_modes)
    for slot in range(6):
        sign = 1.0 if slot % 2 else -1.0
        own_modes[slot, 0:6, :] = jnp.where(present, sign * got.traces[:, slot, 0, :], 0.0)

    fetch.load.wait()

    fetch.flex.wait()
    fetch.bmap.wait()

    def cut_flex(i, carry):
        at = pl.ds(pl.multiple_of(i * FACE, FACE), FACE)
        high, low = split(got.flex[at, :])
        s.flex2[at, 0:NB] = high
        s.flex2[at, NB : 2 * NB] = low
        sign = lax.convert_element_type(2 * lax.rem(i, 2) - 1, F32)
        spot = i * FACE + lax.broadcasted_iota(jnp.int32, (FACE, NB), 0)
        s.pick[at, :] = jnp.where(got.bmap[...] == spot, sign, 0.0).astype(BF16)
        return carry

    lax.fori_loop(0, 6, cut_flex, 0)

    pl.semaphore_wait(barrier, len(peers))

    def coarse_y(k):
        c = eight(s.plane[k][...]).reshape(nx * nz * 8, FACE)
        part = fold(dot(s.inverse[...], wide(c)), ny * 8).reshape(ny, 8, FACE)
        for j in range(ny):
            s.part[k][j] = part[j, 0:6]
        return to_each(s.part[k], s.gy[k])

    def graph(k, slot):
        own = eight(s.ring[k][0])
        near = eight(s.ring[k][1 + slot])
        high, low = halves(jnp.concatenate([own, near], axis=0))
        stack = jnp.concatenate([high, high, low, jnp.zeros((FACE - 48, FACE), F32)], axis=0).astype(BF16)
        return dot(s.basis[slot], stack)

    def modes_dot(z):
        return fold(dot(s.modes2[...], wide(z)), 8)[0:6]

    def apply(x):
        return fold(dot(s.op2[...], wide(x)), NB)

    def spread(r, k):
        own = None
        for slot in range(6):
            part = fold(dot(s.both2[slot], wide(r[slot_rows(slot), :])), 16)
            own = part[0:6] if own is None else own + part[0:6]
            s.share[k][slot] = part[8:14]
        came = to_faces(lambda slot: s.share[k].at[slot], s.shares[k])
        s.mine[k][...] = own
        return came

    def gathered(k):
        return s.mine[k][...] + total(s.shares[k])

    def stencil(k):
        return fold(dot(s.stencil2[...], wide(eight(s.ring[k][...]).reshape(256, FACE))), 8)[0:6]

    def operate(k, x, load=None):
        out = apply(x)
        for slot in range(6):
            part = out[slot_rows(slot), :]
            if load is not None:
                part = (1.0 if slot % 2 else -1.0) * face(load, slot) - part
            s.out[k][slot] = part
        return to_faces(lambda slot: s.out[k].at[slot], s.halo[k])

    def assembled(k):
        return (s.out[k][...] + s.halo[k][...]).reshape(NB, FACE)

    came_cut = to_each(s.cut, s.all_cut)
    came_plane = to_plane(got.load[:, 0, :], s.plane[0])
    came_modes = to_faces(lambda slot: own_modes.at[slot], s.near_modes)

    modes = jnp.concatenate([own_modes[slot] for slot in range(6)], axis=1)
    s.modes2[...] = jnp.concatenate(halves(modes), axis=0).astype(BF16)
    for k in (0, 1, 2, 3, STORED_STEP):
        tail = s.ring[k].shape
        s.ring[k][len(RING) :] = jnp.zeros((tail[0] - len(RING), *tail[1:]), F32)

    def pick_rows(i, carry):
        at = pl.multiple_of(i * FACE, FACE)
        out = dot(s.pick[pl.ds(at, FACE), :], s.flex2[...])
        s.half[pl.ds(at, FACE), :] = out[:, 0:NB].astype(BF16)
        s.half[pl.ds(NB + at, FACE), :] = out[:, NB : 2 * NB].astype(BF16)
        return carry

    def pick_columns(i, carry):
        at = pl.ds(pl.multiple_of(i * 2 * FACE, 2 * FACE), 2 * FACE)
        out = lax.dot_general(s.half[at, :], s.pick[...], (((1,), (1,)), ((), ())), preferred_element_type=F32)
        s.op2[at, :] = out.astype(BF16)
        return carry

    lax.fori_loop(0, 6, pick_rows, 0)
    lax.fori_loop(0, 3, pick_columns, 0)

    came_cut()
    wide_cut = eight(s.all_cut[...]).reshape(ny * 8, s.all_cut.shape[-1])
    col = lax.broadcasted_iota(jnp.int32, (256, 256), 1)
    row = lax.broadcasted_iota(jnp.int32, (256, 256), 0)
    place = lax.rem(lax.div(col, 8), nx) * group + lax.div(col, 8 * nx) * 6 + lax.rem(col, 8)
    pick = jnp.where((row == place) & (lax.rem(col, 8) < 6), 1.0, 0.0).astype(BF16)
    s.inverse[...] = dot(jnp.concatenate(split(wide_cut), axis=0), pick).astype(BF16)

    came_plane()
    came_y = coarse_y(0)

    lax.fori_loop(3, 6, pick_columns, 0)
    came_modes()
    for slot in range(6):
        own, near = own_modes[slot], s.near_modes[slot]
        high, low = halves(jnp.concatenate([own, near], axis=0))
        s.both2[slot] = jnp.concatenate([high, low], axis=0).astype(BF16)
        tall = jnp.concatenate([high, low, high, jnp.zeros((FACE - 48, FACE), F32)], axis=0)
        s.basis[slot] = tall.T.astype(BF16)
        blank = [own] + [jnp.zeros((8, FACE), F32)] * 15
        blank[1 + slot] = near
        s.field_g[slot_rows(slot), :] = jnp.concatenate(blank, axis=0).T
    came_share = spread(apply(s.field_g[...]), 0)
    fetch.disp.wait()
    signed = [(1.0 if slot % 2 else -1.0) * face(got.disp, slot) for slot in range(6)]
    came_load = spread(jnp.concatenate(signed, axis=0), 1)
    came_y()
    came_ring = to_ring(total(s.gy[0]), s.ring[0])

    came_share()
    lane = lax.broadcasted_iota(jnp.int32, (8, FACE), 1)
    parts = [jnp.zeros((8, FACE), F32)] * 2
    for j, base in enumerate((ZERO, *ACROSS)):
        source = eight(s.mine[0][...] if j == 0 else s.shares[0][j - 1])
        for b, step in enumerate((ZERO, *ACROSS)):
            to = RING.index(plus(base, step))
            moved = pltpu.roll(source, (8 * (to % 16) - 8 * b) % FACE, 1)
            parts[to // 16] = parts[to // 16] + jnp.where(lax.div(lane, 8) == to % 16, moved, 0.0)
    s.stencil2[...] = jnp.concatenate(halves(jnp.concatenate(parts, axis=1)), axis=0).astype(BF16)
    came_load()
    came_ring()
    came_plane = to_plane(gathered(1) - stencil(0), s.plane[1])

    lam, w, z, zd, paw = s.lam, s.w, s.z, s.zd, s.paw
    for slot in range(6):
        lam[slot_rows(slot), :] = graph(0, slot)
    came_halo = operate(1, lam[...], got.disp)
    fetch.dirs.wait()
    fetch.curv.wait()
    fetch.images.wait()
    s.scale[...] = jnp.ones_like(s.scale)
    s.scale[0:1, 0:STORED] = got.curv[...]
    inverse_curv = 1.0 / s.scale[0:1, :]
    for slot in range(6):
        tall = jnp.concatenate([got.dirs[slot], jnp.zeros((FACE - STORED, FACE), F32)], axis=0)
        s.field_d[slot_rows(slot), :] = tall.T * inverse_curv
    came_halo_d = operate(0, s.field_d[...])
    came_plane()
    came_y = coarse_y(1)
    came_halo()
    z[...] = assembled(1)
    came_share = spread(apply(z[...]), 2)
    came_halo_d()
    zd[...] = assembled(0)
    came_plane_d = to_plane(modes_dot(zd[...]), s.plane[STORED_STEP])
    s.dirs3[...] = thrice(s.field_d[...])
    modes_of_images = None
    for slot in range(6):
        tall = jnp.concatenate([own_modes[slot], jnp.zeros((FACE - 8, FACE), F32)], axis=0)
        part = lax.dot_general(
            got.images[slot],
            tall,
            (((1,), (1,)), ((), ())),
            precision=lax.Precision.HIGHEST,
            preferred_element_type=F32,
        )
        modes_of_images = part if slot == 0 else modes_of_images + part
        if slot % 2:
            s.images2[slot // 2] = jnp.concatenate(halves(got.images[slot]), axis=0).astype(BF16)
    s.images2[3] = jnp.concatenate(halves(modes_of_images), axis=0).astype(BF16)

    class StoredSums:
        def __init__(self, j, field, alpha):
            self.j = j
            parts = [field[slot_rows(slot), :] for slot in (1, 3, 5)]
            parts.append(jnp.concatenate([eight(-alpha), jnp.zeros((FACE - 8, FACE), F32)], axis=0))
            out = None
            for i, part in enumerate(parts):
                term = dot(s.images2[i], wide(part))
                out = term if out is None else out + term
            flat, cut = fold(out, STORED), STORED // ny
            for i in range(ny):
                s.sums[j][i] = flat[i * cut : (i + 1) * cut]
            self.came = to_each(s.sums[j], s.sums_y[j])

        def share(self):
            self.came()
            self.came = to_plane(total(s.sums_y[self.j]), s.sums_plane[self.j])

        def collect(self):
            self.came()
            self.came = to_all(total(s.sums_plane[self.j]), s.sums_all[self.j])

        def result(self):
            self.came()
            return jnp.concatenate([s.sums_all[self.j][i] for i in range(ny)], axis=0)

    came_y()
    alpha = total(s.gy[1])
    came_ring = to_ring(alpha, s.ring[1])
    sums_w = StoredSums(0, z[...], alpha)
    came_share()
    start = gathered(2)
    came_ring()
    came_plane = to_plane(start - stencil(1), s.plane[2])
    for slot in range(6):
        w[slot_rows(slot), :] = face(z, slot) - graph(1, slot)

    def odd_dot(a, b):
        out = None
        for slot in (1, 3, 5):
            part = jnp.sum(face(a, slot) * face(b, slot), axis=0, keepdims=True)
            out = part if out is None else out + part
        return out

    def superstep(k, v, pairs, came_plane, sums):
        j = k - 3
        came_pairs, came_d, came_share, sums_d, sums_z = None, None, None, None, None
        if pairs:
            lines = [odd_dot(a, b) for a, b in pairs]
            came_pairs = to_all(jnp.concatenate(lines, axis=0), s.pairs_y[j])
        sums[0].share()
        came_halo = operate(k, v[...])
        if k == 2:
            came_plane_d()
            came_y_d = coarse_y(STORED_STEP)
        if k == 4:
            came_pairs()
            came_pairs = to_plane(total(s.pairs_y[j]), s.pairs_plane[j])
        came_plane()
        came_y = coarse_y(k)
        if k == 3:
            came_pairs()
            came_pairs = to_plane(total(s.pairs_y[j]), s.pairs_plane[j])
        for each in sums:
            each.collect()
        if k == 2:
            came_d = spread(apply(zd[...]), 3)
        came_halo()
        z[...] = assembled(k)
        if k == 2:
            came_y_d()
            alpha = total(s.gy[STORED_STEP])
            came_ring_d = to_ring(alpha, s.ring[STORED_STEP])
            sums_d = StoredSums(1, zd[...], alpha)
        if k < 4:
            came_share = spread(apply(z[...]), k + 2)
        came_y()
        alpha = total(s.gy[k])
        came_ring = to_ring(alpha, s.ring[k], len(RING) if k < 4 else 7)
        if k < 4:
            sums_z = StoredSums(k, z[...], alpha)
        if k == 2:
            sums_d.share()
            came_d()
            came_ring_d()
        if k < 4:
            came_share()
        return came_ring, came_pairs, [x for x in (sums_z, sums_d) if x is not None]

    def stored_part(gram):
        high, low = halves(gram)
        return jnp.concatenate([high, high, low, jnp.zeros((8, FACE), F32)], axis=0).astype(BF16)

    p, q = s.p, s.q
    came_ring, _, later = superstep(2, w, (), came_plane, [sums_w])
    modes_pad3 = thrice(eight(gathered(3) - stencil(STORED_STEP)))
    gram = sums_w.result()
    stack = stored_part(gram)
    modes_off = gathered(4) - dot(modes_pad3, stack)[0:6]
    came_ring()
    change = stencil(2)
    modes_q = modes_off - change
    modes_paw = gathered(4) - change
    came_plane = to_plane(modes_q, s.plane[3])
    for slot in range(6):
        at = slot_rows(slot)
        paw[at, :] = face(z, slot) - graph(2, slot)
        s.pad3[at, :] = thrice(face(zd, slot) - graph(STORED_STEP, slot))
    q[0][...] = paw[...] - dot(s.pad3[...], stack)
    p[0][...] = w[...] - dot(s.dirs3[...], stack)

    own, curves = [], []
    for k in range(2):
        pairs = [(p[k], q[k]), (p[k], w), (q[k], w), (q[k], q[k])]
        pairs += [(q[j], q[k]) for j in range(k)]
        came_ring, came_pairs, latest = superstep(3 + k, q[k], pairs, came_plane, later)
        came_pairs()
        sums = total(s.pairs_plane[k])
        lines = [sums[j : j + 1] for j in range(len(pairs))]
        if k == 0:
            gram_paw = later[0].result()
            gram_pad3 = thrice(later[1].result())
            gram_q = gram_paw - dot(gram_pad3, stack)
        else:
            gram_paw = gram_paw - rate * later[0].result()
            gram_q = gram_paw - dot(gram_pad3, stack) - gammas[0] * gram_q
        later = latest
        curves.append(lines[0])
        rate = lines[1] / lines[0]
        own = [own[j] - rate * lines[4 + j] for j in range(k)] + [lines[2] - rate * lines[3]]
        gammas = [own[j] / curves[j] for j in range(k + 1)]
        gram = gram - rate * gram_q
        stack = stored_part(gram)
        if k == 0:
            modes_off = modes_paw - rate * gathered(5) - dot(modes_pad3, stack)[0:6] - gammas[0] * modes_q
        w[...] = w[...] - rate * q[k][...]
        new = w[...] - dot(s.dirs3[...], stack)
        off = dot(s.pad3[...], stack)
        for j in range(k + 1):
            new = new - p[j][...] * gammas[j]
            off = off + q[j][...] * gammas[j]
        p[k + 1][...] = new
        lam[...] = lam[...] + rate * p[k][...]
        if k == 0:
            q[1][...] = paw[...] - rate * z[...] - off
            came_ring()
            came_plane = to_plane(modes_off + rate * stencil(3), s.plane[4])
            for slot in range(6):
                at = slot_rows(slot)
                change = rate * graph(3, slot)
                paw[at, :] = paw[at, :] - rate * face(z, slot) + change
                q[1][at, :] = q[1][at, :] + change

    over = rate * jnp.sum(modes_dot(p[2][...]) * s.ring[4][0], axis=0, keepdims=True)
    q[2][...] = paw[...] - off
    for slot in (1, 3, 5):
        known = face(q[2], slot) - rate * face(z, slot)
        over = over + jnp.sum(face(p[2], slot) * known, axis=0, keepdims=True)
    lines = jnp.concatenate([over, odd_dot(p[2], w)], axis=0)
    came_end = to_plane(lines, s.end_plane)
    came_ring()
    for slot in range(6):
        at = slot_rows(slot)
        image_out[at, :] = q[2][at, :] - rate * (face(z, slot) - graph(4, slot))

    lam_out[...] = lam[...]
    dir_out[...] = p[2][...]
    res_out[...] = w[...]
    came_end()
    to_all(total(s.end_plane), s.end_gy)()
    lines = total(s.end_gy)
    rate_out[...] = lines[1:2] / lines[0:1]

    for sem, ref in unsent:
        wait_bytes(ref, sem)


def per_device(sizes, disp, load, flex, bmap, counts, traces, rows, dirs, images, curv):
    nx, ny, nz = sizes
    vmem = pltpu.VMEM
    given = dict(
        rows=rows.reshape(6, 1, -1),
        load=load.reshape(6, 1, FACE),
        counts=counts.reshape(1, 1),
        traces=traces.reshape(6, 6, 1, FACE),
        flex=flex.reshape(NB, NB),
        bmap=bmap.reshape(1, NB),
        disp=disp.reshape(NB, FACE),
        dirs=dirs.reshape(STORED, 6, FACE).swapaxes(0, 1),
        curv=curv.reshape(1, STORED),
        images=images.reshape(STORED, 6, FACE).swapaxes(0, 1),
    )
    field = vmem((NB, FACE), F32)
    blocks = lambda n, width=FACE, rows=6: vmem((n, rows, width), F32)
    scratch = dict(
        given={name: vmem(x.shape, x.dtype) for name, x in given.items()},
        flex2=vmem((NB, 2 * NB), BF16),
        pick=vmem((NB, NB), BF16),
        half=vmem((2 * NB, NB), BF16),
        op2=vmem((2 * NB, NB), BF16),
        own_rows=vmem((6, 6 * nx * ny * nz), F32),
        cut=blocks(ny, 256),
        all_cut=blocks(ny, 256),
        inverse=vmem((2 * ny * 8, nx * nz * 8), BF16),
        own_modes=blocks(6, rows=8),
        near_modes=blocks(6, rows=8),
        modes2=vmem((16, NB), BF16),
        both2=vmem((6, 32, FACE), BF16),
        stencil2=vmem((16, 256), BF16),
        basis=vmem((6, FACE, FACE), BF16),
        scale=vmem((8, FACE), F32),
        dirs3=vmem((NB, FACE), BF16),
        pad3=vmem((NB, FACE), BF16),
        images2=vmem((4, 2 * STORED, FACE), BF16),
        end_plane=blocks(nx * nz, rows=2),
        end_gy=blocks(ny, rows=2),
        lam=field,
        w=field,
        z=field,
        zd=field,
        field_d=field,
        field_g=field,
        paw=field,
        p=[field] * 3,
        q=[field] * 3,
        out=[vmem((6, FACE, FACE), F32)] * STEPS,
        halo=[vmem((6, FACE, FACE), F32)] * STEPS,
        plane=[blocks(nx * nz)] * STEPS,
        part=[blocks(ny)] * STEPS,
        gy=[blocks(ny)] * STEPS,
        ring=[blocks(32)] * STEPS,
        share=[blocks(6)] * 6,
        shares=[blocks(6)] * 6,
        mine=[vmem((6, FACE), F32)] * 6,
        sums=[blocks(ny, rows=STORED // ny)] * 4,
        sums_y=[blocks(ny, rows=STORED // ny)] * 4,
        sums_plane=[blocks(nx * nz, rows=STORED // ny)] * 4,
        sums_all=[blocks(ny, rows=STORED // ny)] * 4,
        pairs_y=[blocks(ny, rows=4 + k) for k in range(2)],
        pairs_plane=[blocks(nx * nz, rows=4 + k) for k in range(2)],
        local=pltpu.SemaphoreType.DMA((len(given),)),
        sent=pltpu.SemaphoreType.DMA((64,)),
        came=pltpu.SemaphoreType.DMA((64,)),
    )
    leaves, tree = jax.tree.flatten(scratch, is_leaf=lambda x: not isinstance(x, (dict, list)))

    def body(*refs):
        cut = len(given)
        held = SimpleNamespace(**jax.tree.unflatten(tree, refs[cut + 5 :]))
        kernel(sizes, dict(zip(given, refs[:cut])), *refs[cut : cut + 5], held)

    inside = pl.BlockSpec(memory_space=pltpu.VMEM)
    outside = pl.BlockSpec(memory_space=pltpu.HBM)
    lam, direction, res, image, rate = pl.pallas_call(
        body,
        out_shape=[vmem((NB, FACE), F32)] * 4 + [vmem((1, FACE), F32)],
        in_specs=[outside] * len(given),
        out_specs=[inside] * 5,
        scratch_shapes=leaves,
        compiler_params=pltpu.CompilerParams(
            collective_id=0, has_side_effects=True, vmem_limit_bytes=56 * 1024 * 1024
        ),
        name="feti",
    )(*given.values())
    shape = (1, 1, 1, 6, FACE, FACE)
    return (lam + rate * direction).reshape(shape), (res - rate * image).reshape(shape)


def solution(mesh):
    sizes = tuple(mesh.shape[a] for a in AXES)
    cut = P("gx", "gy", "gz")
    return jax.shard_map(
        functools.partial(per_device, sizes),
        mesh=mesh,
        in_specs=(cut,) * 9 + (P(),),
        out_specs=(cut, cut),
        check_vma=False,
    )
```

```python
import functools
from types import SimpleNamespace

import jax
import jax.numpy as jnp
from jax import lax
from jax.experimental import pallas as pl
from jax.experimental.pallas import tpu as pltpu
from jax.sharding import PartitionSpec as P

F32, BF16 = jnp.float32, jnp.bfloat16
GX, GY, GZ = AXES = ("gx", "gy", "gz")
FACE = 128
NB = 6 * FACE
STORED = 40
STEPS = 6
STORED_STEP = 5
ODD_FIRST = (1, 3, 5, 0, 2, 4)
ACROSS = tuple(tuple((1 if slot % 2 else -1) if axis == slot // 2 else 0 for axis in range(3)) for slot in range(6))
ZERO = (0, 0, 0)


def plus(a, b):
    return tuple(i + j for i, j in zip(a, b))


RING = tuple(dict.fromkeys((ZERO, *ACROSS, *(plus(a, b) for a in ACROSS for b in ACROSS))))


def dot(a, b):
    return jnp.dot(a, b, preferred_element_type=F32)


def split(x):
    high = x.astype(BF16)
    return high, (x - high.astype(F32)).astype(BF16)


def wide(x):
    return jnp.concatenate(split(x), axis=1)


def fold(product, rows):
    half = product.shape[1] // 2
    return (product[:rows, :half] + product[:rows, half:]) + product[rows:, :half]


def thrice(x):
    high, low = split(x)
    high, low = high.astype(F32), low.astype(F32)
    return (high + pltpu.roll(low, STORED, 1) + pltpu.roll(high, 2 * STORED, 1)).astype(BF16)


def kernel(sizes, given, lam_out, dir_out, res_out, image_out, rate_out, s):
    nx, ny, nz = sizes
    me = dict(zip(AXES, (lax.axis_index(a) for a in AXES)))
    count = dict(zip(AXES, sizes))
    mesh_id = pl.DeviceIdType.MESH

    def other(axis, delta):
        return lax.rem(me[axis] + (count[axis] + delta), count[axis])

    def at_offset(offset):
        return {axis: other(axis, d) for axis, d in zip(AXES, offset) if d}

    def nearness(offset):
        x, y, z = (min(d % n, -d % n) for d, n in zip(offset, sizes))
        return -(x / 2 + y + z)

    plane = sorted(((dx, 0, dz) for dx in range(nx) for dz in range(nz) if dx or dz), key=nearness)
    line = sorted(((0, dy, 0) for dy in range(1, ny)), key=nearness)
    corner = [o for o in RING if o[1] and (o[0] or o[2])]

    barrier = pltpu.get_barrier_semaphore()
    peers = [at_offset(o) for o in line + plane + corner]
    for peer in peers:
        pl.semaphore_signal(barrier, inc=1, device_id=peer, device_id_type=mesh_id)

    got = s.given
    fetch = {
        name: pltpu.make_async_copy(given[name], got[name], s.local.at[j]) for j, name in enumerate(given)
    }
    for copy in fetch.values():
        copy.start()
    fetch, got = SimpleNamespace(**fetch), SimpleNamespace(**got)

    used = [0]
    unsent = []

    def phase():
        used[0] += 1
        return s.sent.at[used[0] - 1], s.came.at[used[0] - 1]

    def wait_bytes(ref, sem):
        pltpu.make_async_copy(ref, ref, sem).wait()

    def send(src, dst, sems, target):
        pltpu.make_async_remote_copy(
            src_ref=src, dst_ref=dst, send_sem=sems[0], recv_sem=sems[1], device_id=target, device_id_type=mesh_id
        ).start()

    def finish(sems, ref):
        unsent.append((sems[0], ref))
        return lambda: wait_bytes(ref, sems[1])

    def to_faces(piece, dst):
        sems = phase()
        for slot in (2, 3, 4, 5, 0, 1):
            send(piece(slot), dst.at[slot ^ 1], sems, at_offset(ACROSS[slot]))
        return finish(sems, dst)

    def to_all(value, dst):
        sems = phase()
        dst[me[GY]] = value
        for _, delta, _ in line:
            send(dst.at[me[GY]], dst.at[me[GY]], sems, {GY: other(GY, delta)})
        return finish(sems, dst.at[pl.ds(0, ny - 1)])

    def to_each(src, dst):
        sems = phase()
        for _, delta, _ in line:
            peer = other(GY, delta)
            send(src.at[peer], dst.at[me[GY]], sems, {GY: peer})
        dst[me[GY]] = src[me[GY]]
        return finish(sems, dst.at[pl.ds(0, ny - 1)])

    def to_plane(value, dst):
        spot = me[GZ] * nx + me[GX]
        dst[spot] = value
        sems = phase()
        for o in plane:
            send(dst.at[spot], dst.at[spot], sems, at_offset(o))
        return finish(sems, dst.at[pl.ds(0, len(plane))])

    def to_ring(value, dst, reach=len(RING)):
        dst[0] = value
        sems = phase()
        for j in sorted(range(1, reach), key=lambda j: nearness(RING[j])):
            send(dst.at[0], dst.at[j], sems, at_offset(tuple(-d for d in RING[j])))
        return finish(sems, dst.at[pl.ds(1, reach - 1)])

    def total(buf):
        out = buf[0]
        for j in range(1, buf.shape[0]):
            out = out + buf[j]
        return out

    def halves(x):
        high, low = split(x)
        return high.astype(F32), low.astype(F32)

    def eight(x):
        shape = list(x.shape)
        shape[-2] = 8 - shape[-2]
        return jnp.concatenate([x, jnp.zeros(shape, F32)], axis=x.ndim - 2)

    def slot_rows(slot):
        return slice(slot * FACE, (slot + 1) * FACE)

    def face(ref, slot):
        return ref[slot_rows(slot), :]

    group = nz * 6
    s.cut[...] = jnp.zeros_like(s.cut)
    fetch.rows.wait()
    s.own_rows[...] = got.rows[:, 0, :]
    for j in range(ny):
        for i in range(nx):
            at = (i * ny + j) * group
            s.cut[j, :, i * group : (i + 1) * group] = s.own_rows[:, at : at + group]

    fetch.counts.wait()
    fetch.traces.wait()
    present = lax.broadcasted_iota(jnp.int32, (6, FACE), 0) < got.counts[...]
    own_modes = s.own_modes
    own_modes[...] = jnp.zeros_like(own_modes)
    for slot in range(6):
        sign = 1.0 if slot % 2 else -1.0
        own_modes[slot, 0:6, :] = jnp.where(present, sign * got.traces[:, slot, 0, :], 0.0)

    fetch.load.wait()

    fetch.flex.wait()
    fetch.bmap.wait()

    def cut_flex(i, carry):
        at = pl.ds(pl.multiple_of(i * FACE, FACE), FACE)
        high, low = split(got.flex[at, :])
        s.flex2[at, 0:NB] = high
        s.flex2[at, NB : 2 * NB] = low
        sign = lax.convert_element_type(2 * lax.rem(i, 2) - 1, F32)
        spot = i * FACE + lax.broadcasted_iota(jnp.int32, (FACE, NB), 0)
        s.pick[at, :] = jnp.where(got.bmap[...] == spot, sign, 0.0).astype(BF16)
        return carry

    def pick_rows(i, carry):
        at = pl.multiple_of(i * 2 * FACE, 2 * FACE)
        out = dot(s.pick[pl.ds(at, 2 * FACE), :], s.flex2[...])
        s.half[pl.ds(at, 2 * FACE), :] = out[:, 0:NB].astype(BF16)
        s.half[pl.ds(NB + at, 2 * FACE), :] = out[:, NB : 2 * NB].astype(BF16)
        return carry

    lax.fori_loop(0, 6, cut_flex, 0)

    pl.semaphore_wait(barrier, len(peers))

    def coarse_y(k):
        c = eight(s.plane[k][...]).reshape(nx * nz * 8, FACE)
        part = fold(dot(s.inverse[...], wide(c)), ny * 8).reshape(ny, 8, FACE)
        for j in range(ny):
            s.part[k][j] = part[j, 0:6]
        return to_each(s.part[k], s.gy[k])

    def graph(k, slot):
        own = eight(s.ring[k][0])
        near = eight(s.ring[k][1 + slot])
        high, low = halves(jnp.concatenate([own, near], axis=0))
        stack = jnp.concatenate([high, high, low, jnp.zeros((FACE - 48, FACE), F32)], axis=0).astype(BF16)
        return dot(s.basis[slot], stack)

    def modes_dot(z):
        return fold(dot(s.modes2[...], wide(z)), 8)[0:6]

    def apply(x):
        return fold(dot(s.op2[...], wide(x)), NB)

    def spread(r, k):
        own = None
        for slot in range(6):
            part = fold(dot(s.both2[slot], wide(r[slot_rows(slot), :])), 16)
            own = part[0:6] if own is None else own + part[0:6]
            s.share[k][slot] = part[8:14]
        came = to_faces(lambda slot: s.share[k].at[slot], s.shares[k])
        s.mine[k][...] = own
        return came

    def gathered(k):
        return s.mine[k][...] + total(s.shares[k])

    def stencil(k):
        return fold(dot(s.stencil2[...], wide(eight(s.ring[k][...]).reshape(256, FACE))), 8)[0:6]

    def operate(k, x, load=None):
        out = apply(x)
        for slot in range(6):
            part = out[slot_rows(slot), :]
            if load is not None:
                part = (1.0 if slot % 2 else -1.0) * face(load, slot) - part
            s.out[k][slot] = part
        return to_faces(lambda slot: s.out[k].at[slot], s.halo[k])

    def assembled(k):
        return (s.out[k][...] + s.halo[k][...]).reshape(NB, FACE)

    came_cut = to_each(s.cut, s.all_cut)
    came_plane = to_plane(got.load[:, 0, :], s.plane[0])
    came_modes = to_faces(lambda slot: own_modes.at[slot], s.near_modes)

    modes = jnp.concatenate([own_modes[slot] for slot in range(6)], axis=1)
    s.modes2[...] = jnp.concatenate(halves(modes), axis=0).astype(BF16)
    for k in (0, 1, 2, 3, STORED_STEP):
        tail = s.ring[k].shape
        s.ring[k][len(RING) :] = jnp.zeros((tail[0] - len(RING), *tail[1:]), F32)

    def pick_columns(i, carry):
        at = pl.ds(pl.multiple_of(i * 4 * FACE, 4 * FACE), 4 * FACE)
        out = lax.dot_general(s.half[at, :], s.pick[...], (((1,), (1,)), ((), ())), preferred_element_type=F32)
        s.op2[at, :] = out.astype(BF16)
        return carry

    lax.fori_loop(0, 3, pick_rows, 0)
    lax.fori_loop(0, 2, pick_columns, 0)

    came_cut()
    wide_cut = eight(s.all_cut[...]).reshape(ny * 8, s.all_cut.shape[-1])
    col = lax.broadcasted_iota(jnp.int32, (256, 256), 1)
    row = lax.broadcasted_iota(jnp.int32, (256, 256), 0)
    place = lax.rem(lax.div(col, 8), nx) * group + lax.div(col, 8 * nx) * 6 + lax.rem(col, 8)
    pick = jnp.where((row == place) & (lax.rem(col, 8) < 6), 1.0, 0.0).astype(BF16)
    s.inverse[...] = dot(jnp.concatenate(split(wide_cut), axis=0), pick).astype(BF16)

    came_plane()
    came_y = coarse_y(0)

    lax.fori_loop(2, 3, pick_columns, 0)
    came_modes()
    for slot in range(6):
        own, near = own_modes[slot], s.near_modes[slot]
        high, low = halves(jnp.concatenate([own, near], axis=0))
        s.both2[slot] = jnp.concatenate([high, low], axis=0).astype(BF16)
        tall = jnp.concatenate([high, low, high, jnp.zeros((FACE - 48, FACE), F32)], axis=0)
        s.basis[slot] = tall.T.astype(BF16)
        blank = [own] + [jnp.zeros((8, FACE), F32)] * 15
        blank[1 + slot] = near
        s.field_g[slot_rows(slot), :] = jnp.concatenate(blank, axis=0).T
    came_share = spread(apply(s.field_g[...]), 0)
    fetch.disp.wait()
    signed = [(1.0 if slot % 2 else -1.0) * face(got.disp, slot) for slot in range(6)]
    came_load = spread(jnp.concatenate(signed, axis=0), 1)
    came_y()
    came_ring = to_ring(total(s.gy[0]), s.ring[0])

    came_share()
    lane = lax.broadcasted_iota(jnp.int32, (8, FACE), 1)
    parts = [jnp.zeros((8, FACE), F32)] * 2
    for j, base in enumerate((ZERO, *ACROSS)):
        source = eight(s.mine[0][...] if j == 0 else s.shares[0][j - 1])
        for b, step in enumerate((ZERO, *ACROSS)):
            to = RING.index(plus(base, step))
            moved = pltpu.roll(source, (8 * (to % 16) - 8 * b) % FACE, 1)
            parts[to // 16] = parts[to // 16] + jnp.where(lax.div(lane, 8) == to % 16, moved, 0.0)
    s.stencil2[...] = jnp.concatenate(halves(jnp.concatenate(parts, axis=1)), axis=0).astype(BF16)
    came_load()
    came_ring()
    came_plane = to_plane(gathered(1) - stencil(0), s.plane[1])

    lam, w, z, zd, paw = s.lam, s.w, s.z, s.zd, s.paw
    for slot in range(6):
        lam[slot_rows(slot), :] = graph(0, slot)
    came_halo = operate(1, lam[...], got.disp)
    fetch.dirs.wait()
    fetch.curv.wait()
    fetch.images.wait()
    s.scale[...] = jnp.ones_like(s.scale)
    s.scale[0:1, 0:STORED] = got.curv[...]
    inverse_curv = 1.0 / s.scale[0:1, :]
    for slot in range(6):
        tall = jnp.concatenate([got.dirs[slot], jnp.zeros((FACE - STORED, FACE), F32)], axis=0)
        s.field_d[slot_rows(slot), :] = tall.T * inverse_curv
    came_halo_d = operate(0, s.field_d[...])
    came_plane()
    came_y = coarse_y(1)
    came_halo()
    z[...] = assembled(1)
    came_share = spread(apply(z[...]), 2)
    came_halo_d()
    zd[...] = assembled(0)
    came_plane_d = to_plane(modes_dot(zd[...]), s.plane[STORED_STEP])
    s.dirs3[...] = thrice(s.field_d[...])
    modes_of_images = None
    for slot in range(6):
        tall = jnp.concatenate([own_modes[slot], jnp.zeros((FACE - 8, FACE), F32)], axis=0)
        part = lax.dot_general(
            got.images[slot],
            tall,
            (((1,), (1,)), ((), ())),
            precision=lax.Precision.HIGHEST,
            preferred_element_type=F32,
        )
        modes_of_images = part if slot == 0 else modes_of_images + part
        if slot % 2:
            s.images2[slot // 2] = jnp.concatenate(halves(got.images[slot]), axis=0).astype(BF16)
    s.images2[3] = jnp.concatenate(halves(modes_of_images), axis=0).astype(BF16)

    class StoredSums:
        def __init__(self, j, field, alpha):
            self.j = j
            parts = [field[slot_rows(slot), :] for slot in (1, 3, 5)]
            parts.append(jnp.concatenate([eight(-alpha), jnp.zeros((FACE - 8, FACE), F32)], axis=0))
            out = None
            for i, part in enumerate(parts):
                term = dot(s.images2[i], wide(part))
                out = term if out is None else out + term
            flat, cut = fold(out, STORED), STORED // ny
            for i in range(ny):
                s.sums[j][i] = flat[i * cut : (i + 1) * cut]
            self.came = to_each(s.sums[j], s.sums_y[j])

        def share(self):
            self.came()
            self.came = to_plane(total(s.sums_y[self.j]), s.sums_plane[self.j])

        def collect(self):
            self.came()
            self.came = to_all(total(s.sums_plane[self.j]), s.sums_all[self.j])

        def result(self):
            self.came()
            return jnp.concatenate([s.sums_all[self.j][i] for i in range(ny)], axis=0)

    came_y()
    alpha = total(s.gy[1])
    came_ring = to_ring(alpha, s.ring[1])
    sums_w = StoredSums(0, z[...], alpha)
    came_share()
    start = gathered(2)
    came_ring()
    came_plane = to_plane(start - stencil(1), s.plane[2])
    for slot in range(6):
        w[slot_rows(slot), :] = face(z, slot) - graph(1, slot)

    def odd_dot(a, b):
        out = None
        for slot in (1, 3, 5):
            part = jnp.sum(face(a, slot) * face(b, slot), axis=0, keepdims=True)
            out = part if out is None else out + part
        return out

    modes_made = []

    def superstep(k, v, pairs, came_plane, sums):
        j = k - 3
        came_pairs, came_d, came_share, sums_d, sums_z = None, None, None, None, None
        if pairs:
            lines = [odd_dot(a, b) for a, b in pairs]
            came_pairs = to_all(jnp.concatenate(lines, axis=0), s.pairs_y[j])
        sums[0].share()
        came_halo = operate(k, v[...])
        if k == 2:
            came_plane_d()
            came_y_d = coarse_y(STORED_STEP)
        if k == 4:
            came_pairs()
            came_pairs = to_plane(total(s.pairs_y[j]), s.pairs_plane[j])
        came_plane()
        came_y = coarse_y(k)
        if k == 3:
            came_pairs()
            came_pairs = to_plane(total(s.pairs_y[j]), s.pairs_plane[j])
        for each in sums:
            each.collect()
        if k == 2:
            came_d = spread(apply(zd[...]), 3)
        came_halo()
        z[...] = assembled(k)
        if k == 2:
            came_y_d()
            alpha = total(s.gy[STORED_STEP])
            came_ring_d = to_ring(alpha, s.ring[STORED_STEP])
            sums_d = StoredSums(1, zd[...], alpha)
        if k < 4:
            came_share = spread(apply(z[...]), k + 2)
        else:
            modes_made.extend(modes_dot(x[...]) for x in (w, s.q[1], s.p[0], s.p[1]))
            modes_made.append(thrice(eight(modes_dot(s.field_d[...]))))
        came_y()
        alpha = total(s.gy[k])
        came_ring = to_ring(alpha, s.ring[k], len(RING) if k < 4 else 7)
        if k < 4:
            sums_z = StoredSums(k, z[...], alpha)
        if k == 2:
            sums_d.share()
            came_d()
            came_ring_d()
        if k < 4:
            came_share()
        return came_ring, came_pairs, [x for x in (sums_z, sums_d) if x is not None]

    def stored_part(gram):
        high, low = halves(gram)
        return jnp.concatenate([high, high, low, jnp.zeros((8, FACE), F32)], axis=0).astype(BF16)

    p, q = s.p, s.q
    came_ring, _, later = superstep(2, w, (), came_plane, [sums_w])
    modes_pad3 = thrice(eight(gathered(3) - stencil(STORED_STEP)))
    gram = sums_w.result()
    stack = stored_part(gram)
    modes_off = gathered(4) - dot(modes_pad3, stack)[0:6]
    came_ring()
    change = stencil(2)
    modes_q = modes_off - change
    modes_paw = gathered(4) - change
    came_plane = to_plane(modes_q, s.plane[3])
    for slot in range(6):
        at = slot_rows(slot)
        paw[at, :] = face(z, slot) - graph(2, slot)
        s.pad3[at, :] = thrice(face(zd, slot) - graph(STORED_STEP, slot))
    q[0][...] = paw[...] - dot(s.pad3[...], stack)
    p[0][...] = w[...] - dot(s.dirs3[...], stack)

    def step(slot, rate, gammas, stack):
        at = slot_rows(slot)
        w[at, :] = w[at, :] - rate * q[1][at, :]
        new = w[at, :] - dot(s.dirs3[at, :], stack)
        off = dot(s.pad3[at, :], stack)
        for j in range(2):
            new = new - p[j][at, :] * gammas[j]
            off = off + q[j][at, :] * gammas[j]
        p[2][at, :] = new
        q[2][at, :] = paw[at, :] - off - rate * z[at, :]

    own, curves = [], []
    for k in range(2):
        pairs = [(p[k], q[k]), (p[k], w), (q[k], w), (q[k], q[k])]
        pairs += [(q[j], q[k]) for j in range(k)]
        came_ring, came_pairs, latest = superstep(3 + k, q[k], pairs, came_plane, later)
        came_pairs()
        sums = total(s.pairs_plane[k])
        lines = [sums[j : j + 1] for j in range(len(pairs))]
        if k == 0:
            gram_paw = later[0].result()
            gram_pad3 = thrice(later[1].result())
            gram_q = gram_paw - dot(gram_pad3, stack)
        else:
            gram_paw = gram_paw - rate * later[0].result()
            gram_q = gram_paw - dot(gram_pad3, stack) - gammas[0] * gram_q
        later = latest
        curves.append(lines[0])
        rate = lines[1] / lines[0]
        own = [own[j] - rate * lines[4 + j] for j in range(k)] + [lines[2] - rate * lines[3]]
        gammas = [own[j] / curves[j] for j in range(k + 1)]
        gram = gram - rate * gram_q
        stack = stored_part(gram)
        if k == 0:
            modes_off = modes_paw - rate * gathered(5) - dot(modes_pad3, stack)[0:6] - gammas[0] * modes_q
        if k == 1:
            break
        w[...] = w[...] - rate * q[0][...]
        p[1][...] = w[...] - dot(s.dirs3[...], stack) - p[0][...] * gammas[0]
        q[1][...] = paw[...] - rate * z[...] - dot(s.pad3[...], stack) - q[0][...] * gammas[0]
        lam[...] = lam[...] + rate * p[0][...]
        came_ring()
        came_plane = to_plane(modes_off + rate * stencil(3), s.plane[4])
        for slot in ODD_FIRST:
            at = slot_rows(slot)
            change = rate * graph(3, slot)
            paw[at, :] = paw[at, :] - rate * face(z, slot) + change
            q[1][at, :] = q[1][at, :] + change

    modes_p = modes_made[0] - rate * modes_made[1] - gammas[0] * modes_made[2] - gammas[1] * modes_made[3]
    modes_p = modes_p - dot(modes_made[4], stack)[0:6]
    over = rate * jnp.sum(modes_p * s.ring[4][0], axis=0, keepdims=True)
    for slot in ODD_FIRST[:3]:
        step(slot, rate, gammas, stack)
    lines = jnp.concatenate([over + odd_dot(p[2], q[2]), odd_dot(p[2], w)], axis=0)
    came_end = to_plane(lines, s.end_plane)
    for slot in ODD_FIRST[3:]:
        step(slot, rate, gammas, stack)
    lam[...] = lam[...] + rate * p[1][...]
    came_ring()
    for slot in range(6):
        at = slot_rows(slot)
        image_out[at, :] = q[2][at, :] + rate * graph(4, slot)

    lam_out[...] = lam[...]
    dir_out[...] = p[2][...]
    res_out[...] = w[...]
    came_end()
    to_all(total(s.end_plane), s.end_gy)()
    lines = total(s.end_gy)
    rate_out[...] = lines[1:2] / lines[0:1]

    for sem, ref in unsent:
        wait_bytes(ref, sem)


def per_device(sizes, disp, load, flex, bmap, counts, traces, rows, dirs, images, curv):
    nx, ny, nz = sizes
    vmem = pltpu.VMEM
    given = dict(
        rows=rows.reshape(6, 1, -1),
        load=load.reshape(6, 1, FACE),
        counts=counts.reshape(1, 1),
        traces=traces.reshape(6, 6, 1, FACE),
        flex=flex.reshape(NB, NB),
        bmap=bmap.reshape(1, NB),
        disp=disp.reshape(NB, FACE),
        dirs=dirs.reshape(STORED, 6, FACE).swapaxes(0, 1),
        curv=curv.reshape(1, STORED),
        images=images.reshape(STORED, 6, FACE).swapaxes(0, 1),
    )
    field = vmem((NB, FACE), F32)
    blocks = lambda n, width=FACE, rows=6: vmem((n, rows, width), F32)
    scratch = dict(
        given={name: vmem(x.shape, x.dtype) for name, x in given.items()},
        flex2=vmem((NB, 2 * NB), BF16),
        pick=vmem((NB, NB), BF16),
        half=vmem((2 * NB, NB), BF16),
        op2=vmem((2 * NB, NB), BF16),
        own_rows=vmem((6, 6 * nx * ny * nz), F32),
        cut=blocks(ny, 256),
        all_cut=blocks(ny, 256),
        inverse=vmem((2 * ny * 8, nx * nz * 8), BF16),
        own_modes=blocks(6, rows=8),
        near_modes=blocks(6, rows=8),
        modes2=vmem((16, NB), BF16),
        both2=vmem((6, 32, FACE), BF16),
        stencil2=vmem((16, 256), BF16),
        basis=vmem((6, FACE, FACE), BF16),
        scale=vmem((8, FACE), F32),
        dirs3=vmem((NB, FACE), BF16),
        pad3=vmem((NB, FACE), BF16),
        images2=vmem((4, 2 * STORED, FACE), BF16),
        end_plane=blocks(nx * nz, rows=2),
        end_gy=blocks(ny, rows=2),
        lam=field,
        w=field,
        z=field,
        zd=field,
        field_d=field,
        field_g=field,
        paw=field,
        p=[field] * 3,
        q=[field] * 3,
        out=[vmem((6, FACE, FACE), F32)] * STEPS,
        halo=[vmem((6, FACE, FACE), F32)] * STEPS,
        plane=[blocks(nx * nz)] * STEPS,
        part=[blocks(ny)] * STEPS,
        gy=[blocks(ny)] * STEPS,
        ring=[blocks(32)] * STEPS,
        share=[blocks(6)] * 6,
        shares=[blocks(6)] * 6,
        mine=[vmem((6, FACE), F32)] * 6,
        sums=[blocks(ny, rows=STORED // ny)] * 4,
        sums_y=[blocks(ny, rows=STORED // ny)] * 4,
        sums_plane=[blocks(nx * nz, rows=STORED // ny)] * 4,
        sums_all=[blocks(ny, rows=STORED // ny)] * 4,
        pairs_y=[blocks(ny, rows=4 + k) for k in range(2)],
        pairs_plane=[blocks(nx * nz, rows=4 + k) for k in range(2)],
        local=pltpu.SemaphoreType.DMA((len(given),)),
        sent=pltpu.SemaphoreType.DMA((64,)),
        came=pltpu.SemaphoreType.DMA((64,)),
    )
    leaves, tree = jax.tree.flatten(scratch, is_leaf=lambda x: not isinstance(x, (dict, list)))

    def body(*refs):
        cut = len(given)
        held = SimpleNamespace(**jax.tree.unflatten(tree, refs[cut + 5 :]))
        kernel(sizes, dict(zip(given, refs[:cut])), *refs[cut : cut + 5], held)

    inside = pl.BlockSpec(memory_space=pltpu.VMEM)
    outside = pl.BlockSpec(memory_space=pltpu.HBM)
    lam, direction, res, image, rate = pl.pallas_call(
        body,
        out_shape=[vmem((NB, FACE), F32)] * 4 + [vmem((1, FACE), F32)],
        in_specs=[outside] * len(given),
        out_specs=[inside] * 5,
        scratch_shapes=leaves,
        compiler_params=pltpu.CompilerParams(
            collective_id=0, has_side_effects=True, vmem_limit_bytes=56 * 1024 * 1024
        ),
        name="feti",
    )(*given.values())
    shape = (1, 1, 1, 6, FACE, FACE)
    return (lam + rate * direction).reshape(shape), (res - rate * image).reshape(shape)


def solution(mesh):
    sizes = tuple(mesh.shape[a] for a in AXES)
    cut = P("gx", "gy", "gz")
    return jax.shard_map(
        functools.partial(per_device, sizes),
        mesh=mesh,
        in_specs=(cut,) * 9 + (P(),),
        out_specs=(cut, cut),
        check_vma=False,
    )
```
